256 devices in a mesh: seq: 64 (over z, y, x_hi), head: 4 (over x_lo, core).
Axes of the slice: x: 4 (x_hi: 2, x_lo: 2; x = x_hi * 2 + x_lo), y: 4, z: 8, core: 2. Of those that a mesh axis runs over, the one named last changes fastest.
Arguments:
- queries: bfloat16 [8192, 4096], P('seq', 'head'), may hold values from -12 to 12
- keys: bfloat16 [8192, 2048], P('seq', 'head'), may hold values from -12 to 12
- values: bfloat16 [8192, 2048], P('seq', 'head'), may hold values from -6 to 6
- block_order: int32 [128], replicated, may hold values from 0 to 127, each once
Outputs:
- attn: bfloat16 [8192, 4096], P(('seq', 'head'))
- lse: float32 [16, 8192], P('head', 'seq')
The draws below stay inside these ranges and needn't reach their ends.
Inputs may be any that keep to these rules, and one draw needn't show every extreme that they name: device-order block j (rows j * 64 to j * 64 + 63) holds sequence positions block_order[j] * 64 onward, in order.
All inputs are finite; a program needn't handle non-finite values.
Results may differ from the reference program's by a relative error of at most 0.006.
Values may be sent and summed in bfloat16 or wider, within the bound.
A program may use at most 128 MiB of HBM per device.

```python
import jax
import jax.numpy as jnp
from jax import lax

HQ = 16
KEY_VALUE_HEADS = 8
HEAD_SIZE = 256
S_DEV = 128
QUERY_GROUP = 2
BLK = 64
NB = 128
SEQUENCE_TOKENS = 8192
N_SEQ = 64


def draw_queries(key, part):
    base_offset = jax.random.truncated_normal(jax.random.fold_in(key, 1), -3.0, 3.0, (SEQUENCE_TOKENS, HQ * HEAD_SIZE), jnp.float32)
    return base_offset.astype(jnp.bfloat16)


def draw_keys(key, part):
    base_offset = jax.random.truncated_normal(jax.random.fold_in(key, 2), -3.0, 3.0, (SEQUENCE_TOKENS, KEY_VALUE_HEADS * HEAD_SIZE), jnp.float32)
    return base_offset.astype(jnp.bfloat16)


def level_of(stream_key, extent, shards, smallest, top_value):
    def one(axis_at, blocks):
        heights = jax.random.uniform(jax.random.fold_in(jax.random.fold_in(stream_key, 6), axis_at), (blocks,), jnp.float32, smallest / len(shards), top_value / len(shards))
        return jnp.repeat(jnp.exp(heights), extent[axis_at] // blocks).reshape((-1,) + (1,) * (len(extent) - axis_at - 1))

    factor_of = one(*shards[0])
    for cut in shards[1:]:
        factor_of = factor_of * one(*cut)
    return factor_of


def scatter_about(key, shape, spread, most, pieces=(), held_as=jnp.bfloat16):
    array = jax.random.normal(key, shape, jnp.float32) * spread
    if len(pieces) > 0:
        array = level_of(key, shape, pieces, -0.22, 0.18) * array
    return jnp.clip(array, min=-most, max=most).astype(held_as)


def setup_inputs(seed: int = 0) -> dict:
    key_of = jax.random.split(jax.random.key(seed), 5)
    queries = draw_queries(jax.random.fold_in(key_of[4], 71), 0)
    keys = draw_keys(jax.random.fold_in(key_of[4], 71), 0)
    values = scatter_about(key_of[2], (SEQUENCE_TOKENS, KEY_VALUE_HEADS * HEAD_SIZE), 1.0, 6.0, ((0, 64), (1, 4)))
    block_order = jax.random.permutation(key_of[3], NB).astype(jnp.int32)
    return {"queries": queries, "keys": keys, "values": values, "block_order": block_order}


def reference(queries, keys, values, block_order):
    rows = jnp.arange(SEQUENCE_TOKENS, dtype=jnp.int32)
    pos = (block_order[rows // BLK] * BLK + rows % BLK).astype(jnp.int32)
    query_head_count = queries.reshape(SEQUENCE_TOKENS, KEY_VALUE_HEADS, QUERY_GROUP, HEAD_SIZE)
    key_single = keys.reshape(SEQUENCE_TOKENS, KEY_VALUE_HEADS, HEAD_SIZE).astype(jnp.float32)
    value_single = values.reshape(SEQUENCE_TOKENS, KEY_VALUE_HEADS, HEAD_SIZE).astype(jnp.float32)
    scale = HEAD_SIZE ** -0.5

    def one_block(index):
        start = (index * S_DEV).astype(jnp.int32)
        query_block = lax.dynamic_slice_in_dim(query_head_count, start, S_DEV, 0).astype(jnp.float32)
        query_pos = lax.dynamic_slice_in_dim(pos, start, S_DEV, 0)
        scores = jnp.einsum('qhgd,khd->hgqk', query_block, key_single) * scale
        allowed = pos[None, :] <= query_pos[:, None]
        scores = jnp.where(allowed, scores, -1e30)
        row_max = jnp.max(scores, axis=-1)
        weights = jnp.where(allowed, jnp.exp(scores - row_max[..., None]), 0.0)
        total = jnp.sum(weights, axis=-1)
        rounded = lax.optimization_barrier(weights.astype(jnp.bfloat16))
        summed = jnp.einsum('hgqk,khd->qhgd', rounded.astype(jnp.float32), value_single)
        output = summed / jnp.transpose(total, (2, 0, 1))[..., None]
        return output.reshape(S_DEV, HQ * HEAD_SIZE).astype(jnp.bfloat16), (row_max + jnp.log(total)).reshape(HQ, S_DEV)

    outputs, sums = lax.map(one_block, jnp.arange(N_SEQ, dtype=jnp.int32))
    attn = outputs.reshape(SEQUENCE_TOKENS, HQ * HEAD_SIZE)
    lse = jnp.transpose(sums, (1, 0, 2)).reshape(HQ, SEQUENCE_TOKENS)
    return attn, lse
```

```python
import functools

import jax
import jax.numpy as jnp
from jax import lax
from jax.experimental import pallas as pl
from jax.experimental.pallas import tpu as pltpu
from jax.sharding import PartitionSpec as P

MESH = pl.DeviceIdType.MESH
HEAD = 256
ROWS = 128
BLK = 64
NZ, NY = 8, 4
NEG = -1e30
FLOOR = -1e6
LOG2E = 1.4426950408889634
LN2 = 0.6931471805599453
F32 = jnp.float32
BF16 = jnp.bfloat16

RIGHT_SLOTS = (0, 1, 2, 3, 7)
LEFT_SLOTS = (0, 4, 5, 6, 7)
SLOT_DZ = (0, -1, -2, -3, 1, 2, 3, 4)
QUERY_DY = (0, -1, 1, 2)


def combine(parts):
    top = functools.reduce(jnp.maximum, [lse for _, lse in parts])
    weights = [jnp.exp2(lse - top) for _, lse in parts]
    total = functools.reduce(jnp.add, weights)
    scale = 1.0 / total
    out = functools.reduce(jnp.add, [o.astype(F32) * (w * scale) for (o, _), w in zip(parts, weights)])
    return out, top + jnp.log2(total)


def kernel(q_ref, k_ref, v_ref, order_ref, attn_ref, lse_ref,
           qbuf, kbuf, vbuf, vm, vsw, qpos, acc, mx, ls,
           osend, lsend, orecv, lrecv, obuf, abuf, lxs, lxr,
           local_sem, send_sem, recv_sem):
    s = lax.axis_index("seq")
    g = lax.axis_index("head")
    z = s // (2 * NY)
    y = (s // 2) % NY
    c = s % 2

    def at(dz, dy):
        return (((z + dz + NZ) % NZ) * NY + (y + dy + NY) % NY) * 2 + c

    partner = (s + 1 - 2 * c, g)
    up, down = (at(1, 0), g), (at(-1, 0), g)
    fore, back = (at(0, 1), g), (at(0, -1), g)

    loads = [
        pltpu.make_async_copy(v_ref, vm, local_sem.at[0]),
        pltpu.make_async_copy(k_ref.at[:, pl.ds(pl.multiple_of(c * HEAD, HEAD), HEAD)], kbuf.at[0, pl.ds(0, ROWS), :], local_sem.at[1]),
    ]
    for hd in range(2):
        loads.append(pltpu.make_async_copy(
            q_ref.at[:, pl.ds(pl.multiple_of(c * 2 * HEAD + hd * HEAD, HEAD), HEAD)],
            qbuf.at[0, pl.ds(hd * ROWS, ROWS), :], local_sem.at[2 + hd]))
    for copy in loads:
        copy.start()

    line = []
    for r in range(2):
        for e in range(4):
            if r or e:
                line.append(((s if r == 0 else s + 1 - 2 * c), (g + e) % 4))
    barrier = pltpu.get_barrier_semaphore()
    for peer in line + [up, down, fore, back]:
        pl.semaphore_signal(barrier, inc=1, device_id=peer, device_id_type=MESH)

    table = {}

    def message(name, src, dst, device):
        i = len(table)
        table[name] = pltpu.make_async_remote_copy(
            src_ref=src, dst_ref=dst, send_sem=send_sem.at[i], recv_sem=recv_sem.at[i],
            device_id=device, device_id_type=MESH)

    other = 1 - c
    for hd in range(2):
        message(("xq", hd), q_ref.at[:, pl.ds(pl.multiple_of(other * 2 * HEAD + hd * HEAD, HEAD), HEAD)],
                qbuf.at[1, pl.ds(hd * ROWS, ROWS), :], partner)
    message("xk", k_ref.at[:, pl.ds(pl.multiple_of(other * HEAD, HEAD), HEAD)], kbuf.at[0, pl.ds(ROWS, ROWS), :], partner)
    message("xv", vsw, vbuf.at[0, :, pl.ds(ROWS, ROWS)], partner)
    for h in range(2):
        def kpart(slot):
            return kbuf.at[slot, pl.ds(h * ROWS, ROWS), :]

        def vpart(slot):
            return vbuf.at[slot, :, pl.ds(h * ROWS, ROWS)]

        for t in range(1, 5):
            message(("rk", h, t), kpart(RIGHT_SLOTS[t - 1]), kpart(RIGHT_SLOTS[t]), up)
            message(("lv", h, t), vpart(LEFT_SLOTS[t - 1]), vpart(LEFT_SLOTS[t]), down)
            if t < 4:
                message(("lk", h, t), kpart(LEFT_SLOTS[t - 1]), kpart(LEFT_SLOTS[t]), down)
                message(("rv", h, t), vpart(RIGHT_SLOTS[t - 1]), vpart(RIGHT_SLOTS[t]), up)

        def qpart(slot, hd):
            return qbuf.at[slot * 2 + h, pl.ds(hd * ROWS, ROWS), :]

        for hd in range(2):
            message(("qr", h, hd), qpart(0, hd), qpart(1, hd), fore)
            message(("ql", h, hd), qpart(0, hd), qpart(2, hd), back)
        message(("qrr", h), qpart(1, 0), qpart(3, 0), fore)
        message(("qll", h), qpart(2, 1), qpart(3, 1), back)
    for n in range(6):
        device = fore if n % 2 == 0 else back
        message(("o", n), osend.at[n], orecv.at[n], device)
        message(("l", n), lsend.at[n], lrecv.at[n], device)
    message("lx", lxs, lxr, partner)

    def line_copy(r, e, index, sender_c, sender_g, device):
        rows = pl.ds(pl.multiple_of(((sender_g + e) % 4) * 32, 32), 32)
        cols = pl.ds(pl.multiple_of((2 * sender_g + sender_c) * 2 * HEAD, 2 * HEAD), 2 * HEAD)
        return pltpu.make_async_remote_copy(
            src_ref=obuf.at[r, rows, :], dst_ref=abuf.at[:, cols],
            send_sem=send_sem.at[index], recv_sem=recv_sem.at[index], device_id=device, device_id_type=MESH)

    base = len(table)
    line_out, line_in = {}, {}
    for r in range(2):
        for e in range(4):
            if r or e:
                index = base + r * 4 + e
                there = s if r == 0 else s + 1 - 2 * c
                line_out[r, e] = line_copy(r, e, index, c, g, (there, (g + e) % 4))
                line_in[r, e] = line_copy(r, e, index, c if r == 0 else other, (g + 4 - e) % 4, (there, (g + e) % 4))

    started = []

    def send(name):
        table[name].start()
        started.append(table[name])

    def arrive(name):
        table[name].wait_recv()

    loads[0].wait()

    def flipped(column):
        v = vm[:, pl.ds(pl.multiple_of(column * HEAD, HEAD), HEAD)]
        return v.astype(F32).T.astype(BF16)

    vbuf[0, :, 0:ROWS] = flipped(c)
    vsw[...] = flipped(other)

    lane = lax.broadcasted_iota(jnp.int32, (8, HEAD), 1)
    for slot in range(4):
        for h in range(2):
            origin = (z * NY + (y + QUERY_DY[slot] + NY) % NY) * 2 + (c if h == 0 else other)
            first, second = order_ref[2 * origin] * BLK, order_ref[2 * origin + 1] * BLK
            inside = lane % ROWS
            qpos[slot * 2 + h] = jnp.where(inside < BLK, first + inside, second + inside - BLK)

    def key_bases(slot):
        out = []
        for h in range(2):
            origin = (((z + SLOT_DZ[slot] + NZ) % NZ) * NY + y) * 2 + (c if h == 0 else other)
            out += [order_ref[2 * origin] * BLK, order_ref[2 * origin + 1] * BLK]
        return out

    iota = lax.broadcasted_iota(jnp.int32, (BLK, HEAD), 0)

    def step(i, slots, bases, first):
        q = qbuf[i]
        position = qpos[i, 0:1, :]
        scores = []
        for slot, base4 in zip(slots, bases):
            raw = lax.dot_general(kbuf[slot], q, (((1,), (1,)), ((), ())), preferred_element_type=F32)
            parts = [
                jnp.where(iota <= position - base4[b], raw[b * BLK:(b + 1) * BLK] * (LOG2E / 16.0), NEG)
                for b in range(4)
            ]
            scores.append(jnp.concatenate(parts, axis=0))
        best = functools.reduce(jnp.maximum, [jnp.max(t.reshape(32, 8, HEAD), axis=0) for t in scores])
        best = jnp.max(best, axis=0, keepdims=True)
        old = jnp.full((1, HEAD), FLOOR, F32) if first else mx[i, 0:1, :]
        fresh = jnp.maximum(old, best)
        weights = [jnp.exp2(t - fresh) for t in scores]
        sums = functools.reduce(jnp.add, [jnp.sum(w.reshape(32, 8, HEAD), axis=0) for w in weights])
        update = functools.reduce(jnp.add, [
            lax.dot_general(vbuf[slot], w.astype(BF16), (((1,), (0,)), ((), ())), preferred_element_type=F32)
            for slot, w in zip(slots, weights)
        ])
        if first:
            return update, fresh, sums
        factor = jnp.exp2(old - fresh)
        return acc[i] * factor + update, fresh, ls[i] * factor + sums

    def attend(tiles, slots, first=False):
        bases = [key_bases(slot) for slot in slots]
        start, stop = tiles

        def body(j, carry):
            for i in (start + 2 * j, start + 2 * j + 1):
                a, m, l = step(i, slots, bases, first)
                acc[i] = a
                mx[i] = jnp.broadcast_to(m, (8, HEAD))
                ls[i] = l
            return carry

        lax.fori_loop(0, (stop - start) // 2, body, 0)

    def finish(i, slots, bases):
        a, m, l8 = step(i, slots, bases, False)
        l = jnp.sum(l8, axis=0, keepdims=True)
        some = l > 0.0
        inverse = jnp.where(some, 1.0 / jnp.where(some, l, 1.0), 0.0)
        return a * inverse, jnp.where(some, m + jnp.log2(jnp.where(some, l, 1.0)), NEG)

    for copy in loads[1:]:
        copy.wait()
    pl.semaphore_wait(barrier, 11)

    send(("rk", 0, 1))
    send(("lk", 0, 1))
    send(("xq", 0))
    send(("xq", 1))
    for hd in range(2):
        send(("qr", 0, hd))
        send(("ql", 0, hd))
    send(("rv", 0, 1))
    send(("lv", 0, 1))
    send("xk")
    send("xv")

    def ring(h, t):
        arrive(("rk", h, t))
        if t < 4:
            send(("rk", h, t + 1))
            arrive(("lk", h, t))
            if t < 3:
                send(("lk", h, t + 1))
            arrive(("rv", h, t))
            if t < 3:
                send(("rv", h, t + 1))
        arrive(("lv", h, t))
        if t < 4:
            send(("lv", h, t + 1))

    def spread(h):
        for hd in range(2):
            send(("qr", h, hd))
            send(("ql", h, hd))

    def relay(h):
        arrive(("qr", h, 0))
        send(("qrr", h))
        arrive(("ql", h, 1))
        send(("qll", h))
        arrive(("qr", h, 1))
        arrive(("ql", h, 0))

    def relayed(h):
        arrive(("qrr", h))
        arrive(("qll", h))

    relay(0)
    ring(0, 1)
    arrive(("xq", 0))
    arrive(("xq", 1))
    spread(1)
    arrive("xk")
    send(("rk", 1, 1))
    send(("lk", 1, 1))
    ring(0, 2)
    arrive("xv")
    send(("rv", 1, 1))
    send(("lv", 1, 1))
    relayed(0)
    relay(1)
    attend((0, 2), (0,), first=True)
    ring(1, 1)
    ring(0, 3)
    attend((2, 6), (0,), first=True)
    attend((0, 6), (1, 4))
    ring(1, 2)
    ring(0, 4)
    relayed(1)
    attend((6, 8), (0,), first=True)
    attend((6, 8), (1, 4))
    attend((0, 8), (2, 5))
    ring(1, 3)
    attend((0, 8), (3, 6))
    ring(1, 4)

    bases = [key_bases(7)]

    def post(n, o, lse):
        osend[n] = o.astype(BF16)
        lsend[n] = jnp.broadcast_to(lse, (8, HEAD))
        send(("o", n))
        send(("l", n))

    def taken(n):
        arrive(("o", n))
        arrive(("l", n))
        return orecv[n], lrecv[n, 0:1, :]

    post(0, *finish(6, (7,), bases))
    post(1, *finish(7, (7,), bases))
    post(2, *finish(5, (7,), bases))
    post(3, *finish(2, (7,), bases))
    mine = finish(4, (7,), bases)
    post(4, *combine([mine, taken(0)]))
    mine = finish(3, (7,), bases)
    post(5, *combine([mine, taken(1)]))

    def result(r, pieces):
        out, lse = combine(pieces)
        flat = out.T.astype(BF16)
        for hd in range(2):
            obuf[r, :, hd * HEAD:(hd + 1) * HEAD] = flat[hd * ROWS:(hd + 1) * ROWS]
        for e in range(4):
            if r or e:
                line_out[r, e].start()
                started.append(line_out[r, e])
        return lse * LN2

    own = [finish(0, (7,), bases), finish(1, (7,), bases)]
    lse0 = result(0, [own[0], taken(3), taken(4)])
    for hd in range(2):
        lse_ref[pl.ds(2 * c + hd, 1), :] = lse0[:, hd * ROWS:(hd + 1) * ROWS]
    lse1 = result(1, [own[1], taken(2), taken(5)])
    lxs[...] = jnp.concatenate(
        [jnp.broadcast_to(lse1[:, 0:ROWS], (4, ROWS)), jnp.broadcast_to(lse1[:, ROWS:], (4, ROWS))], axis=0)
    send("lx")
    cols = pl.ds(pl.multiple_of((2 * g + c) * 2 * HEAD, 2 * HEAD), 2 * HEAD)
    abuf[:, cols] = obuf[0, pl.ds(pl.multiple_of(g * 32, 32), 32), :]
    arrive("lx")
    for hd in range(2):
        lse_ref[pl.ds(2 * other + hd, 1), :] = lxr[4 * hd:4 * hd + 1, :]
    for copy in line_in.values():
        copy.wait_recv()
    attn_ref[...] = abuf[...]
    for copy in started:
        copy.wait_send()


def local(queries, keys, values, block_order):
    any_space = pl.BlockSpec(memory_space=pl.ANY)
    vmem = pl.BlockSpec(memory_space=pltpu.VMEM)
    return pl.pallas_call(
        kernel,
        out_shape=(
            jax.ShapeDtypeStruct((32, 4096), BF16),
            jax.ShapeDtypeStruct((4, ROWS), F32),
        ),
        in_specs=[any_space, any_space, any_space, pl.BlockSpec(memory_space=pltpu.SMEM)],
        out_specs=(vmem, vmem),
        scratch_shapes=[
            pltpu.VMEM((8, 256, HEAD), BF16),
            pltpu.VMEM((8, 256, HEAD), BF16),
            pltpu.VMEM((8, HEAD, 256), BF16),
            pltpu.VMEM((ROWS, 2 * HEAD), BF16),
            pltpu.VMEM((HEAD, ROWS), BF16),
            pltpu.VMEM((8, 8, HEAD), jnp.int32),
            pltpu.VMEM((8, HEAD, 256), F32),
            pltpu.VMEM((8, 8, 256), F32),
            pltpu.VMEM((8, 8, 256), F32),
            pltpu.VMEM((6, HEAD, 256), BF16),
            pltpu.VMEM((6, 8, 256), F32),
            pltpu.VMEM((6, HEAD, 256), BF16),
            pltpu.VMEM((6, 8, 256), F32),
            pltpu.VMEM((2, ROWS, 2 * HEAD), BF16),
            pltpu.VMEM((32, 4096), BF16),
            pltpu.VMEM((8, ROWS), F32),
            pltpu.VMEM((8, ROWS), F32),
            pltpu.SemaphoreType.DMA((4,)),
            pltpu.SemaphoreType.DMA((72,)),
            pltpu.SemaphoreType.DMA((72,)),
        ],
        compiler_params=pltpu.CompilerParams(collective_id=0, has_side_effects=True, vmem_limit_bytes=60 * 1024 * 1024),
        name="attention",
    )(queries, keys, values, block_order)


def solution(mesh):
    in_specs = (P("seq", "head"), P("seq", "head"), P("seq", "head"), P())
    out_specs = (P(("seq", "head"), None), P("head", "seq"))
    return jax.shard_map(local, mesh=mesh, in_specs=in_specs, out_specs=out_specs, check_vma=False)
```

```python
import functools

import jax
import jax.numpy as jnp
from jax import lax
from jax.experimental import pallas as pl
from jax.experimental.pallas import tpu as pltpu
from jax.sharding import PartitionSpec as P

MESH = pl.DeviceIdType.MESH
HEAD = 256
ROWS = 128
BLK = 64
NZ, NY = 8, 4
NEG = -1e30
BIG = 1e30
SCALE = 1.4426950408889634 / 16.0
FLOOR = -1e6
LN2 = 0.6931471805599453
F32 = jnp.float32
BF16 = jnp.bfloat16

RIGHT_SLOTS = (0, 1, 2, 3, 7)
LEFT_SLOTS = (0, 4, 5, 6, 7)
SLOT_DZ = (0, -1, -2, -3, 1, 2, 3, 4)
QUERY_DY = (0, -1, 1, 2)


def combine(parts):
    top = functools.reduce(jnp.maximum, [lse for _, lse in parts])
    weights = [jnp.exp2(lse - top) for _, lse in parts]
    total = functools.reduce(jnp.add, weights)
    scale = 1.0 / total
    out = functools.reduce(jnp.add, [o.astype(F32) * (w * scale) for (o, _), w in zip(parts, weights)])
    return out, top + jnp.log2(total)


def kernel(q_ref, k_ref, v_ref, order_ref, attn_ref, lse_ref,
           qbuf, kbuf, vbuf, vm, vsw, qpos, acc, mx, ls,
           osend, lsend, orecv, lrecv, obuf, abuf, lxs, lxr, sa, sb, pa, pb, km, qm,
           local_sem, send_sem, recv_sem):
    s = lax.axis_index("seq")
    g = lax.axis_index("head")
    z = s // (2 * NY)
    y = (s // 2) % NY
    c = s % 2

    def at(dz, dy):
        return (((z + dz + NZ) % NZ) * NY + (y + dy + NY) % NY) * 2 + c

    partner = (s + 1 - 2 * c, g)
    up, down = (at(1, 0), g), (at(-1, 0), g)
    fore, back = (at(0, 1), g), (at(0, -1), g)

    loads = [
        pltpu.make_async_copy(v_ref, vm, local_sem.at[0]),
        pltpu.make_async_copy(k_ref.at[:, pl.ds(pl.multiple_of(c * HEAD, HEAD), HEAD)], kbuf.at[0, pl.ds(0, ROWS), :], local_sem.at[1]),
    ]
    for hd in range(2):
        loads.append(pltpu.make_async_copy(
            q_ref.at[:, pl.ds(pl.multiple_of(c * 2 * HEAD + hd * HEAD, HEAD), HEAD)],
            qbuf.at[0, pl.ds(hd * ROWS, ROWS), :], local_sem.at[2 + hd]))
    loads += [
        pltpu.make_async_copy(k_ref.at[:, pl.ds(pl.multiple_of((1 - c) * HEAD, HEAD), HEAD)], km, local_sem.at[4]),
        pltpu.make_async_copy(q_ref.at[:, pl.ds(pl.multiple_of((1 - c) * 2 * HEAD, HEAD), 2 * HEAD)], qm, local_sem.at[5]),
    ]
    for copy in loads:
        copy.start()

    line = []
    for r in range(2):
        for e in range(4):
            if r or e:
                line.append(((s if r == 0 else s + 1 - 2 * c), (g + e) % 4))
    barrier = pltpu.get_barrier_semaphore()
    for peer in line + [up, down, fore, back]:
        pl.semaphore_signal(barrier, inc=1, device_id=peer, device_id_type=MESH)

    table = {}

    def message(name, src, dst, device):
        i = len(table)
        table[name] = pltpu.make_async_remote_copy(
            src_ref=src, dst_ref=dst, send_sem=send_sem.at[i], recv_sem=recv_sem.at[i],
            device_id=device, device_id_type=MESH)

    other = 1 - c
    for hd in range(2):
        message(("xq", hd), qm.at[:, pl.ds(hd * HEAD, HEAD)],
                qbuf.at[4, pl.ds(hd * ROWS, ROWS), :], partner)
    message("xk", km, kbuf.at[0, pl.ds(ROWS, ROWS), :], partner)
    message("xv", vsw, vbuf.at[0, :, pl.ds(ROWS, ROWS)], partner)
    for h in range(2):
        def kpart(slot):
            return kbuf.at[slot, pl.ds(h * ROWS, ROWS), :]

        def vpart(slot):
            return vbuf.at[slot, :, pl.ds(h * ROWS, ROWS)]

        for t in range(1, 5):
            message(("rk", h, t), kpart(RIGHT_SLOTS[t - 1]), kpart(RIGHT_SLOTS[t]), up)
            message(("lv", h, t), vpart(LEFT_SLOTS[t - 1]), vpart(LEFT_SLOTS[t]), down)
            if t < 4:
                message(("lk", h, t), kpart(LEFT_SLOTS[t - 1]), kpart(LEFT_SLOTS[t]), down)
                message(("rv", h, t), vpart(RIGHT_SLOTS[t - 1]), vpart(RIGHT_SLOTS[t]), up)

        def qpart(slot, hd):
            return qbuf.at[h * 4 + slot, pl.ds(hd * ROWS, ROWS), :]

        for hd in range(2):
            message(("qr", h, hd), qpart(0, hd), qpart(1, hd), fore)
            message(("ql", h, hd), qpart(0, hd), qpart(2, hd), back)
        message(("qrr", h), qpart(1, 0), qpart(3, 0), fore)
        message(("qll", h), qpart(2, 1), qpart(3, 1), back)
    for n in range(6):
        device = fore if n % 2 == 0 else back
        message(("o", n), osend.at[n], orecv.at[n], device)
        message(("l", n), lsend.at[n], lrecv.at[n], device)
    message("lx", lxs, lxr, partner)

    def line_copy(r, e, index, sender_c, sender_g, device):
        rows = pl.ds(pl.multiple_of(((sender_g + e) % 4) * 32, 32), 32)
        cols = pl.ds(pl.multiple_of((2 * sender_g + sender_c) * 2 * HEAD, 2 * HEAD), 2 * HEAD)
        return pltpu.make_async_remote_copy(
            src_ref=obuf.at[r, rows, :], dst_ref=abuf.at[:, cols],
            send_sem=send_sem.at[index], recv_sem=recv_sem.at[index], device_id=device, device_id_type=MESH)

    base = len(table)
    line_out, line_in = {}, {}
    for r in range(2):
        for e in range(4):
            if r or e:
                index = base + r * 4 + e
                there = s if r == 0 else s + 1 - 2 * c
                line_out[r, e] = line_copy(r, e, index, c, g, (there, (g + e) % 4))
                line_in[r, e] = line_copy(r, e, index, c if r == 0 else other, (g + 4 - e) % 4, (there, (g + e) % 4))

    started = []

    def send(name):
        table[name].start()
        started.append(table[name])

    def arrive(name):
        table[name].wait_recv()

    loads[0].wait()

    def flipped(column):
        v = vm[:, pl.ds(pl.multiple_of(column * HEAD, HEAD), HEAD)]
        return v.astype(F32).T.astype(BF16)

    vbuf[0, :, 0:ROWS] = flipped(c)
    vsw[...] = flipped(other)

    lane = lax.broadcasted_iota(jnp.int32, (8, HEAD), 1)
    for slot in range(4):
        for h in range(2):
            origin = (z * NY + (y + QUERY_DY[slot] + NY) % NY) * 2 + (c if h == 0 else other)
            first, second = order_ref[2 * origin] * BLK, order_ref[2 * origin + 1] * BLK
            inside = lane % ROWS
            qpos[h * 4 + slot] = jnp.where(inside < BLK, first + inside, second + inside - BLK)

    def key_bases(slot):
        out = []
        for h in range(2):
            origin = (((z + SLOT_DZ[slot] + NZ) % NZ) * NY + y) * 2 + (c if h == 0 else other)
            out += [order_ref[2 * origin] * BLK, order_ref[2 * origin + 1] * BLK]
        return out

    iota = lax.broadcasted_iota(jnp.int32, (BLK, HEAD), 0)

    score_buffers, weight_buffers = (sa, sb), (pa, pb)
    bases_of = {}
    queue = []
    count = [0]

    def stage_scores(item):
        i, slots = item["tile"], item["slots"]
        into = score_buffers[item["turn"] % 2]
        q = qbuf[i]
        for n, slot in enumerate(slots):
            into[n * 256:(n + 1) * 256, :] = lax.dot_general(
                kbuf[slot], q, (((1,), (1,)), ((), ())), preferred_element_type=F32)

    def stage_weights(item):
        i, slots = item["tile"], item["slots"]
        source, into = score_buffers[item["turn"] % 2], weight_buffers[item["turn"] % 2]
        diagonal = slots == (0,) and i in (0, 4)
        first = slots == (0,)
        position = qpos[i, 0:1, :]
        for slot in slots:
            if slot not in bases_of:
                bases_of[slot] = key_bases(slot)
        bases = [base for slot in slots for base in bases_of[slot]]

        def raw(b):
            block = source[b * BLK:(b + 1) * BLK, :]
            return jnp.where(iota <= position - bases[b], block, NEG) if diagonal else block

        old = jnp.full((1, HEAD), FLOOR, F32) if first else mx[i, 0:1, :]
        allowed = [base <= position for base in bases]
        best = functools.reduce(jnp.maximum, [
            jnp.where(allowed[b], jnp.max(raw(b).reshape(8, 8, HEAD), axis=0), NEG) for b in range(len(bases))])
        best = jnp.max(best, axis=0, keepdims=True) * SCALE
        fresh = jnp.maximum(old, best)
        sums = None
        for b in range(len(bases)):
            weights = jnp.exp2(raw(b) * SCALE - jnp.where(allowed[b], fresh, BIG))
            part = jnp.sum(weights.reshape(8, 8, HEAD), axis=0)
            sums = part if sums is None else sums + part
            into[b * BLK:(b + 1) * BLK, :] = weights.astype(BF16)
        if first:
            item["factor"] = None
        else:
            item["factor"] = jnp.exp2(old - fresh)
            sums = ls[i] * item["factor"] + sums
        if item["last"]:
            item["top"], item["sums"] = fresh, sums
        else:
            mx[i] = jnp.broadcast_to(fresh, (8, HEAD))
            ls[i] = sums

    def stage_values(item):
        i, slots = item["tile"], item["slots"]
        source = weight_buffers[item["turn"] % 2]
        update = functools.reduce(jnp.add, [
            lax.dot_general(vbuf[slot], source[n * 256:(n + 1) * 256, :], (((1,), (0,)), ((), ())), preferred_element_type=F32)
            for n, slot in enumerate(slots)
        ])
        if item["factor"] is not None:
            update = acc[i] * item["factor"] + update
        if item["last"]:
            l = jnp.sum(item["sums"], axis=0, keepdims=True)
            some = l > 0.0
            inverse = jnp.where(some, 1.0 / jnp.where(some, l, 1.0), 0.0)
            item["done"](update * inverse, jnp.where(some, item["top"] + jnp.log2(jnp.where(some, l, 1.0)), NEG))
        else:
            acc[i] = update

    def advance():
        if queue and queue[-1]["stage"] == 0:
            stage_scores(queue[-1])
        for item in queue[::-1]:
            if item["stage"] == 1:
                stage_weights(item)
            elif item["stage"] == 2:
                stage_values(item)
        for item in queue:
            item["stage"] += 1
        queue[:] = [item for item in queue if item["stage"] < 3]

    def push(tiles, slots, done=None):
        for i in tiles:
            queue.append({"tile": i, "slots": slots, "turn": count[0], "stage": 0, "last": done is not None, "done": done})
            count[0] += 1
            advance()

    def flush():
        while queue:
            advance()

    for copy in loads[1:]:
        copy.wait()
    pl.semaphore_wait(barrier, 11)

    send(("rk", 0, 1))
    send(("lk", 0, 1))
    send("xk")
    send("xv")
    for hd in range(2):
        send(("qr", 0, hd))
        send(("ql", 0, hd))
    send(("rv", 0, 1))
    send(("lv", 0, 1))
    send(("xq", 0))
    send(("xq", 1))

    def ring_keys(h, t):
        arrive(("rk", h, t))
        if t < 4:
            send(("rk", h, t + 1))
            arrive(("lk", h, t))
            if t < 3:
                send(("lk", h, t + 1))

    def ring_values(h, t):
        arrive(("lv", h, t))
        if t < 4:
            send(("lv", h, t + 1))
            arrive(("rv", h, t))
            if t < 3:
                send(("rv", h, t + 1))

    def ring(h, t):
        ring_keys(h, t)
        ring_values(h, t)

    def spread(hd):
        arrive(("xq", hd))
        send(("qr", 1, hd))
        send(("ql", 1, hd))

    def relay(h, part):
        if part == 0:
            arrive(("qr", h, 0))
            send(("qrr", h))
            arrive(("ql", h, 0))
        else:
            arrive(("ql", h, 1))
            send(("qll", h))
            arrive(("qr", h, 1))

    def relayed(h):
        arrive(("qrr", h))
        arrive(("qll", h))

    def cross_values():
        arrive("xv")
        send(("rv", 1, 1))
        send(("lv", 1, 1))

    def cross_keys():
        arrive("xk")
        send(("rk", 1, 1))
        send(("lk", 1, 1))

    ring_keys(0, 1)
    cross_keys()
    relay(0, 0)
    relay(0, 1)
    ring_values(0, 1)
    cross_values()
    push((0, 1, 2), (0,))
    spread(0)
    spread(1)
    ring_keys(0, 2)
    relayed(0)
    push((3,), (0,))
    ring_keys(1, 1)
    push((4,), (0,))
    ring_values(0, 2)
    relay(1, 0)
    relay(1, 1)
    push((5, 6), (0,))
    ring_values(1, 1)
    push((0, 1, 2, 3), (1, 4))
    ring_keys(0, 3)
    relayed(1)
    push((4, 5), (1, 4))
    ring_keys(1, 2)
    push((6,), (1, 4))
    push((7,), (0,))
    ring_values(0, 3)
    push((7,), (1, 4))
    ring_values(1, 2)
    push((0, 1, 2, 3), (2, 5))
    ring(0, 4)
    push((4, 5), (2, 5))
    ring_keys(1, 3)
    push((6, 7), (2, 5))
    ring_values(1, 3)
    push((0, 1, 2, 3, 4, 5, 6, 7), (3, 6))
    ring(1, 4)

    def post(n, o, lse):
        osend[n] = o.astype(BF16)
        lsend[n] = jnp.broadcast_to(lse, (8, HEAD))
        send(("o", n))
        send(("l", n))

    def taken(n):
        arrive(("o", n))
        arrive(("l", n))
        return orecv[n], lrecv[n, 0:1, :]

    own = {}

    def done_with(tile):
        def done(o, lse):
            if tile in direct:
                post(direct[tile], o, lse)
            elif tile in (2, 5):
                n = 0 if tile == 2 else 1
                post(4 + n, *combine([(o, lse), taken(n)]))
            else:
                own[tile] = (o, lse)
        return done

    direct = {3: 0, 7: 1, 6: 2, 1: 3}
    for tile in (3, 7, 6, 1, 0, 4, 2, 5):
        push((tile,), (7,), done_with(tile))
    flush()

    def result(r, pieces):
        out, lse = combine(pieces)
        flat = out.T.astype(BF16)
        for hd in range(2):
            obuf[r, :, hd * HEAD:(hd + 1) * HEAD] = flat[hd * ROWS:(hd + 1) * ROWS]
        for e in range(4):
            if r or e:
                line_out[r, e].start()
                started.append(line_out[r, e])
        return lse * LN2

    lse0 = result(0, [own[0], taken(3), taken(4)])
    for hd in range(2):
        lse_ref[pl.ds(2 * c + hd, 1), :] = lse0[:, hd * ROWS:(hd + 1) * ROWS]
    lse1 = result(1, [own[4], taken(2), taken(5)])
    lxs[...] = jnp.concatenate(
        [jnp.broadcast_to(lse1[:, 0:ROWS], (4, ROWS)), jnp.broadcast_to(lse1[:, ROWS:], (4, ROWS))], axis=0)
    send("lx")
    cols = pl.ds(pl.multiple_of((2 * g + c) * 2 * HEAD, 2 * HEAD), 2 * HEAD)
    abuf[:, cols] = obuf[0, pl.ds(pl.multiple_of(g * 32, 32), 32), :]
    arrive("lx")
    for hd in range(2):
        lse_ref[pl.ds(2 * other + hd, 1), :] = lxr[4 * hd:4 * hd + 1, :]
    for copy in line_in.values():
        copy.wait_recv()
    attn_ref[...] = abuf[...]
    for copy in started:
        copy.wait_send()


def local(queries, keys, values, block_order):
    any_space = pl.BlockSpec(memory_space=pltpu.HBM)
    vmem = pl.BlockSpec(memory_space=pltpu.VMEM)
    return pl.pallas_call(
        kernel,
        out_shape=(
            jax.ShapeDtypeStruct((32, 4096), BF16),
            jax.ShapeDtypeStruct((4, ROWS), F32),
        ),
        in_specs=[any_space, any_space, any_space, pl.BlockSpec(memory_space=pltpu.SMEM)],
        out_specs=(vmem, vmem),
        scratch_shapes=[
            pltpu.VMEM((8, 256, HEAD), BF16),
            pltpu.VMEM((8, 256, HEAD), BF16),
            pltpu.VMEM((8, HEAD, 256), BF16),
            pltpu.VMEM((ROWS, 2 * HEAD), BF16),
            pltpu.VMEM((HEAD, ROWS), BF16),
            pltpu.VMEM((8, 8, HEAD), jnp.int32),
            pltpu.VMEM((8, HEAD, 256), F32),
            pltpu.VMEM((8, 8, 256), F32),
            pltpu.VMEM((8, 8, 256), F32),
            pltpu.VMEM((6, HEAD, 256), BF16),
            pltpu.VMEM((6, 8, 256), F32),
            pltpu.VMEM((6, HEAD, 256), BF16),
            pltpu.VMEM((6, 8, 256), F32),
            pltpu.VMEM((2, ROWS, 2 * HEAD), BF16),
            pltpu.VMEM((32, 4096), BF16),
            pltpu.VMEM((8, ROWS), F32),
            pltpu.VMEM((8, ROWS), F32),
            pltpu.VMEM((512, HEAD), F32),
            pltpu.VMEM((512, HEAD), F32),
            pltpu.VMEM((512, HEAD), BF16),
            pltpu.VMEM((512, HEAD), BF16),
            pltpu.VMEM((ROWS, HEAD), BF16),
            pltpu.VMEM((ROWS, 2 * HEAD), BF16),
            pltpu.SemaphoreType.DMA((6,)),
            pltpu.SemaphoreType.DMA((72,)),
            pltpu.SemaphoreType.DMA((72,)),
        ],
        compiler_params=pltpu.CompilerParams(collective_id=0, has_side_effects=True, vmem_limit_bytes=24 * 1024 * 1024),
        name="attention",
    )(*[pltpu.with_memory_space_constraint(a, pltpu.HBM) for a in (queries, keys, values, block_order)])


def solution(mesh):
    in_specs = (P("seq", "head"), P("seq", "head"), P("seq", "head"), P())
    out_specs = (P(("seq", "head"), None), P("head", "seq"))
    return jax.shard_map(local, mesh=mesh, in_specs=in_specs, out_specs=out_specs, check_vma=False)
```

```python
import functools

import jax
import jax.numpy as jnp
from jax import lax
from jax.experimental import pallas as pl
from jax.experimental.pallas import tpu as pltpu
from jax.sharding import PartitionSpec as P

MESH = pl.DeviceIdType.MESH
HEAD = 256
ROWS = 128
BLK = 64
NZ, NY = 8, 4
NEG = -1e30
BIG = 1e30
SCALE = 1.4426950408889634 / 16.0
FLOOR = -1e6
LN2 = 0.6931471805599453
F32 = jnp.float32
BF16 = jnp.bfloat16

RIGHT_SLOTS = (0, 1, 2, 3, 7)
LEFT_SLOTS = (0, 4, 5, 6, 7)
SLOT_DZ = (0, -1, -2, -3, 1, 2, 3, 4)
QUERY_DY = (0, -1, 1, 2)


def combine(parts):
    top = functools.reduce(jnp.maximum, [lse for _, lse in parts])
    weights = [jnp.exp2(lse - top) for _, lse in parts]
    total = functools.reduce(jnp.add, weights)
    scale = 1.0 / total
    out = functools.reduce(jnp.add, [o.astype(F32) * (w * scale) for (o, _), w in zip(parts, weights)])
    return out, top + jnp.log2(total)


def kernel(q_ref, k_ref, v_ref, order_hbm, attn_ref, lse_ref,
           qbuf, kbuf, vbuf, vm, vsw, qpos, acc, mx, ls,
           osend, lsend, orecv, lrecv, obuf, abuf, lxs, lxr, sa, sb, pa, pb, km, qm, yard, order_ref,
           local_sem, send_sem, recv_sem):
    s = lax.axis_index("seq")
    g = lax.axis_index("head")
    z = s // (2 * NY)
    y = (s // 2) % NY
    c = s % 2

    def at(dz, dy):
        return (((z + dz + NZ) % NZ) * NY + (y + dy + NY) % NY) * 2 + c

    partner = (s + 1 - 2 * c, g)
    up, down = (at(1, 0), g), (at(-1, 0), g)
    fore, back = (at(0, 1), g), (at(0, -1), g)

    loads = [
        pltpu.make_async_copy(v_ref, vm, local_sem.at[0]),
        pltpu.make_async_copy(k_ref.at[:, pl.ds(pl.multiple_of(c * HEAD, HEAD), HEAD)], kbuf.at[0, pl.ds(0, ROWS), :], local_sem.at[1]),
    ]
    for hd in range(2):
        loads.append(pltpu.make_async_copy(
            q_ref.at[:, pl.ds(pl.multiple_of(c * 2 * HEAD + hd * HEAD, HEAD), HEAD)],
            qbuf.at[0, pl.ds(hd * ROWS, ROWS), :], local_sem.at[2 + hd]))
    loads += [
        pltpu.make_async_copy(k_ref.at[:, pl.ds(pl.multiple_of((1 - c) * HEAD, HEAD), HEAD)], km, local_sem.at[4]),
        pltpu.make_async_copy(q_ref.at[:, pl.ds(pl.multiple_of((1 - c) * 2 * HEAD, HEAD), 2 * HEAD)], qm, local_sem.at[5]),
    ]
    order_load = pltpu.make_async_copy(order_hbm, order_ref, local_sem.at[6])
    for n in (1, 4, 2, 3, 0, 5):
        loads[n].start()
    order_load.start()

    line = []
    for r in range(2):
        for e in range(4):
            if r or e:
                line.append(((s if r == 0 else s + 1 - 2 * c), (g + e) % 4))
    barrier = pltpu.get_barrier_semaphore()
    for peer in line + [up, down, fore, back]:
        pl.semaphore_signal(barrier, inc=1, device_id=peer, device_id_type=MESH)

    table = {}
    recv_slots = {}

    def recv_slot(key):
        return recv_sem.at[recv_slots.setdefault(key, len(recv_slots))]

    def message(name, src, dst, device, group, key=None):
        table[name] = pltpu.make_async_remote_copy(
            src_ref=src, dst_ref=dst, send_sem=send_sem.at[group], recv_sem=recv_slot(name if key is None else key),
            device_id=device, device_id_type=MESH)

    def drain(sem, kib):
        ref = yard.at[pl.ds(0, kib // 4)]
        pltpu.make_async_copy(ref, ref, sem).wait()

    other = 1 - c
    for hd in range(2):
        message(("xq", hd), qm.at[:, pl.ds(hd * HEAD, HEAD)], qbuf.at[4, pl.ds(hd * ROWS, ROWS), :], partner, 1)
    message("xk", km, kbuf.at[0, pl.ds(ROWS, ROWS), :], partner, 1)
    message("xv", vsw, vbuf.at[0, :, pl.ds(ROWS, ROWS)], partner, 1)
    for h in range(2):
        def kpart(slot):
            return kbuf.at[slot, pl.ds(h * ROWS, ROWS), :]

        def vpart(slot):
            return vbuf.at[slot, :, pl.ds(h * ROWS, ROWS)]

        for t in range(1, 5):
            key = ("end", h) if t == 4 else None
            message(("rk", h, t), kpart(RIGHT_SLOTS[t - 1]), kpart(RIGHT_SLOTS[t]), up, 0, key)
            message(("lv", h, t), vpart(LEFT_SLOTS[t - 1]), vpart(LEFT_SLOTS[t]), down, 0, key)
            if t < 4:
                message(("lk", h, t), kpart(LEFT_SLOTS[t - 1]), kpart(LEFT_SLOTS[t]), down, 0)
                message(("rv", h, t), vpart(RIGHT_SLOTS[t - 1]), vpart(RIGHT_SLOTS[t]), up, 0)

        def qpart(slot, hd):
            return qbuf.at[h * 4 + slot, pl.ds(hd * ROWS, ROWS), :]

        message(("qr", h, 0), qpart(0, 0), qpart(1, 0), fore, 1)
        message(("ql", h, 1), qpart(0, 1), qpart(2, 1), back, 1)
        message(("qr", h, 1), qpart(0, 1), qpart(1, 1), fore, 1, ("near", h))
        message(("ql", h, 0), qpart(0, 0), qpart(2, 0), back, 1, ("near", h))
        message(("qrr", h), qpart(1, 0), qpart(3, 0), fore, 1, ("far", h))
        message(("qll", h), qpart(2, 1), qpart(3, 1), back, 1, ("far", h))
    for n in range(6):
        device = fore if n % 2 == 0 else back
        for hd in range(2):
            message(("l", n, hd), lsend.at[2 * n + hd], lrecv.at[2 * n + hd], device, 3, ("taken", n, hd))
            message(("o", n, hd), osend.at[2 * n + hd], orecv.at[2 * n + hd], device, 2, ("taken", n, hd))
    for hd in range(2):
        message(("lx", hd), lxs.at[hd], lxr.at[hd], partner, 3, "lx")
    for r in range(2):
        for e in range(4):
            for hd in range(2):
                if r or e:
                    rows = pl.ds(pl.multiple_of(((g + e) % 4) * 32, 32), 32)
                    cols = pl.ds(pl.multiple_of(((2 * g + c) * 2 + hd) * HEAD, HEAD), HEAD)
                    there = s if r == 0 else s + 1 - 2 * c
                    message(("line", r, e, hd), obuf.at[r, rows, pl.ds(hd * HEAD, HEAD)], abuf.at[:, cols],
                            (there, (g + e) % 4), 3, "line")

    def send(name):
        table[name].start()

    def arrive(name):
        table[name].wait_recv()

    def key_bases(slot):
        out = []
        for h in range(2):
            origin = (((z + SLOT_DZ[slot] + NZ) % NZ) * NY + y) * 2 + (c if h == 0 else other)
            out += [order_ref[2 * origin] * BLK, order_ref[2 * origin + 1] * BLK]
        return out

    iota = lax.broadcasted_iota(jnp.int32, (BLK, HEAD), 0)

    score_buffers, weight_buffers = (sa, sb), (pa, pb)
    bases_of = {}
    queue = []
    count = [0]

    def stage_scores(item):
        i, slots = item["tile"], item["slots"]
        into = score_buffers[item["turn"] % 2]
        q = qbuf[i]
        for n, slot in enumerate(slots):
            into[n * 256:(n + 1) * 256, :] = lax.dot_general(
                kbuf[slot], q, (((1,), (1,)), ((), ())), preferred_element_type=F32)

    def stage_weights(item):
        i, slots = item["tile"], item["slots"]
        source, into = score_buffers[item["turn"] % 2], weight_buffers[item["turn"] % 2]
        diagonal = slots == (0,) and i in (0, 4)
        first = slots == (0,)
        position = qpos[i, 0:1, :]
        for slot in slots:
            if slot not in bases_of:
                bases_of[slot] = key_bases(slot)
        bases = [base for slot in slots for base in bases_of[slot]]

        def raw(b):
            block = source[b * BLK:(b + 1) * BLK, :]
            return jnp.where(iota <= position - bases[b], block, NEG) if diagonal else block

        old = jnp.full((1, HEAD), FLOOR, F32) if first else mx[i, 0:1, :]
        allowed = [base <= position for base in bases]
        best = functools.reduce(jnp.maximum, [
            jnp.where(allowed[b], jnp.max(raw(b).reshape(8, 8, HEAD), axis=0), NEG) for b in range(len(bases))])
        best = jnp.max(best, axis=0, keepdims=True) * SCALE
        fresh = jnp.maximum(old, best)
        sums = None
        for b in range(len(bases)):
            weights = jnp.exp2(raw(b) * SCALE - jnp.where(allowed[b], fresh, BIG))
            part = jnp.sum(weights.reshape(8, 8, HEAD), axis=0)
            sums = part if sums is None else sums + part
            into[b * BLK:(b + 1) * BLK, :] = weights.astype(BF16)
        if first:
            item["factor"] = None
        else:
            item["factor"] = jnp.exp2(old - fresh)
            sums = ls[i] * item["factor"] + sums
        if item["last"]:
            item["top"], item["sums"] = fresh, sums
        else:
            mx[i] = jnp.broadcast_to(fresh, (8, HEAD))
            ls[i] = sums

    def stage_values(item):
        i, slots = item["tile"], item["slots"]
        source = weight_buffers[item["turn"] % 2]
        update = functools.reduce(jnp.add, [
            lax.dot_general(vbuf[slot], source[n * 256:(n + 1) * 256, :], (((1,), (0,)), ((), ())), preferred_element_type=F32)
            for n, slot in enumerate(slots)
        ])
        if item["factor"] is not None:
            update = acc[i] * item["factor"] + update
        if item["last"]:
            l = jnp.sum(item["sums"], axis=0, keepdims=True)
            some = l > 0.0
            inverse = jnp.where(some, 1.0 / jnp.where(some, l, 1.0), 0.0)
            item["done"](update * inverse, jnp.where(some, item["top"] + jnp.log2(jnp.where(some, l, 1.0)), NEG))
        else:
            acc[i] = update

    def advance():
        if queue and queue[-1]["stage"] == 0:
            stage_scores(queue[-1])
        for item in queue[::-1]:
            if item["stage"] == 1:
                stage_weights(item)
            elif item["stage"] == 2:
                stage_values(item)
        for item in queue:
            item["stage"] += 1
        queue[:] = [item for item in queue if item["stage"] < 3]

    def push(tiles, slots, done=None):
        for i in tiles:
            queue.append({"tile": i, "slots": slots, "turn": count[0], "stage": 0, "last": done is not None, "done": done})
            count[0] += 1
            advance()

    def flush():
        while queue:
            advance()

    def first_hop(kind, h):
        send(("r" + kind, h, 1))
        send(("l" + kind, h, 1))

    def ring_keys(h, t):
        arrive(("rk", h, t))
        send(("rk", h, t + 1))
        arrive(("lk", h, t))
        if t < 3:
            send(("lk", h, t + 1))

    def ring_values(h, t):
        arrive(("lv", h, t))
        send(("lv", h, t + 1))
        arrive(("rv", h, t))
        if t < 3:
            send(("rv", h, t + 1))

    def ring_end(h):
        drain(recv_slot(("end", h)), 128)

    def spread(hd):
        arrive(("xq", hd))
        send(("qr", 1, hd))
        send(("ql", 1, hd))

    def relay(h):
        arrive(("qr", h, 0))
        send(("qrr", h))
        arrive(("ql", h, 1))
        send(("qll", h))
        drain(recv_slot(("near", h)), 128)

    def relayed(h):
        drain(recv_slot(("far", h)), 128)

    def cross_values():
        arrive("xv")
        first_hop("v", 1)

    def cross_keys():
        arrive("xk")
        first_hop("k", 1)

    assert len(recv_slots) == 52, len(recv_slots)
    loads[1].wait()
    loads[4].wait()
    pl.semaphore_wait(barrier, 11)
    first_hop("k", 0)
    send("xk")
    for hd in range(2):
        loads[2 + hd].wait()
        send(("qr", 0, hd))
        send(("ql", 0, hd))

    def flipped(column):
        v = vm[:, pl.ds(pl.multiple_of(column * HEAD, HEAD), HEAD)]
        return v.astype(F32).T.astype(BF16)

    loads[0].wait()
    vbuf[0, :, 0:ROWS] = flipped(c)
    vsw[...] = flipped(other)
    order_load.wait()
    lane = lax.broadcasted_iota(jnp.int32, (8, HEAD), 1)
    for slot in range(4):
        for h in range(2):
            origin = (z * NY + (y + QUERY_DY[slot] + NY) % NY) * 2 + (c if h == 0 else other)
            first, second = order_ref[2 * origin] * BLK, order_ref[2 * origin + 1] * BLK
            inside = lane % ROWS
            qpos[h * 4 + slot] = jnp.where(inside < BLK, first + inside, second + inside - BLK)
    send("xv")
    first_hop("v", 0)
    loads[5].wait()
    send(("xq", 0))
    send(("xq", 1))

    ring_keys(0, 1)
    cross_keys()
    relay(0)
    ring_values(0, 1)
    cross_values()
    push((0, 1, 2), (0,))
    spread(0)
    spread(1)
    ring_keys(0, 2)
    relayed(0)
    push((3,), (0,))
    ring_keys(1, 1)
    push((4,), (0,))
    ring_values(0, 2)
    relay(1)
    push((5, 6), (0,))
    ring_values(1, 1)
    push((0, 1, 2, 3), (1, 4))
    ring_keys(0, 3)
    push((4, 5), (1, 4))
    ring_keys(1, 2)
    ring_values(0, 3)
    push((6,), (1, 4))
    ring_values(1, 2)
    relayed(1)
    push((7,), (0,))
    push((7,), (1, 4))
    push((0, 1), (2, 5))
    ring_keys(1, 3)
    push((2, 3, 4), (2, 5))
    ring_values(1, 3)
    push((5, 6, 7), (2, 5))
    push((0, 1, 2, 3, 4, 5, 6, 7), (3, 6))
    ring_end(0)
    ring_end(1)

    def piece(i, hd):
        return acc[i, :, hd * ROWS:(hd + 1) * ROWS], mx[i, 0:1, hd * ROWS:(hd + 1) * ROWS]

    def stage_out(n, hd, o, lse):
        osend[2 * n + hd] = o.astype(BF16)
        lsend[2 * n + hd] = jnp.broadcast_to(lse, (8, ROWS))

    def ship(n, hd):
        send(("l", n, hd))
        send(("o", n, hd))

    def taken(n, hd):
        drain(recv_slot(("taken", n, hd)), 68)
        return orecv[2 * n + hd], lrecv[2 * n + hd, 0:1, :]

    direct = {3: 0, 7: 1, 6: 2, 1: 3}

    def done_with(tile):
        def done(o, lse):
            if tile in direct:
                n = direct[tile]
                for hd in range(2):
                    stage_out(n, hd, o[:, hd * ROWS:(hd + 1) * ROWS], lse[:, hd * ROWS:(hd + 1) * ROWS])
                    if n < 2 or hd == 0:
                        ship(n, hd)
            else:
                acc[tile] = o
                mx[tile] = jnp.broadcast_to(lse, (8, HEAD))
        return done

    for tile in (3, 7, 6, 1, 2, 5, 0, 4):
        push((tile,), (7,), done_with(tile))
    flush()
    for hd in range(2):
        for n, tile in ((0, 2), (1, 5)):
            stage_out(4 + n, hd, *combine([piece(tile, hd), taken(n, hd)]))
            ship(4 + n, hd)
            if hd == 0:
                ship(2 + n, 1)

    def result(r, hd):
        pieces = [piece(0, hd), taken(3, hd), taken(4, hd)] if r == 0 else [piece(4, hd), taken(2, hd), taken(5, hd)]
        out, lse = combine(pieces)
        lse = lse * LN2
        if r:
            lxs[hd] = jnp.broadcast_to(lse, (8, ROWS))
            send(("lx", hd))
        else:
            lse_ref[pl.ds(2 * c + hd, 1), :] = lse
        obuf[r, :, hd * HEAD:(hd + 1) * HEAD] = out.T.astype(BF16)
        for e in range(4):
            if r or e:
                send(("line", r, e, hd))

    for hd in range(2):
        result(0, hd)
        result(1, hd)
    cols = pl.ds(pl.multiple_of((2 * g + c) * 2 * HEAD, 2 * HEAD), 2 * HEAD)
    abuf[:, cols] = obuf[0, pl.ds(pl.multiple_of(g * 32, 32), 32), :]
    drain(recv_slot("lx"), 8)
    for hd in range(2):
        lse_ref[pl.ds(2 * other + hd, 1), :] = lxr[hd, 0:1, :]
    drain(recv_slot("line"), 224)
    attn_ref[...] = abuf[...]
    for group, kib in enumerate((28 * 64, 16 * 64, 12 * 64, 280)):
        drain(send_sem.at[group], kib)


def settle(attn_in, lse_in, attn_out, lse_out, sem):
    copies = [
        pltpu.make_async_copy(attn_in, attn_out, sem.at[0]),
        pltpu.make_async_copy(lse_in, lse_out, sem.at[1]),
    ]
    for copy in copies:
        copy.start()
    for copy in copies:
        copy.wait()


def local(queries, keys, values, block_order):
    hbm = pl.BlockSpec(memory_space=pltpu.HBM)
    vmem = pl.BlockSpec(memory_space=pltpu.VMEM)
    results = pl.pallas_call(
        kernel,
        out_shape=(
            jax.ShapeDtypeStruct((32, 4096), BF16),
            jax.ShapeDtypeStruct((4, ROWS), F32),
        ),
        in_specs=[hbm, hbm, hbm, hbm],
        out_specs=(vmem, vmem),
        scratch_shapes=[
            pltpu.VMEM((8, 256, HEAD), BF16),
            pltpu.VMEM((8, 256, HEAD), BF16),
            pltpu.VMEM((8, HEAD, 256), BF16),
            pltpu.VMEM((ROWS, 2 * HEAD), BF16),
            pltpu.VMEM((HEAD, ROWS), BF16),
            pltpu.VMEM((8, 8, HEAD), jnp.int32),
            pltpu.VMEM((8, HEAD, 256), F32),
            pltpu.VMEM((8, 8, 256), F32),
            pltpu.VMEM((8, 8, 256), F32),
            pltpu.VMEM((12, HEAD, ROWS), BF16),
            pltpu.VMEM((12, 8, ROWS), F32),
            pltpu.VMEM((12, HEAD, ROWS), BF16),
            pltpu.VMEM((12, 8, ROWS), F32),
            pltpu.VMEM((2, ROWS, 2 * HEAD), BF16),
            pltpu.VMEM((32, 4096), BF16),
            pltpu.VMEM((2, 8, ROWS), F32),
            pltpu.VMEM((2, 8, ROWS), F32),
            pltpu.VMEM((512, HEAD), F32),
            pltpu.VMEM((512, HEAD), F32),
            pltpu.VMEM((512, HEAD), BF16),
            pltpu.VMEM((512, HEAD), BF16),
            pltpu.VMEM((ROWS, HEAD), BF16),
            pltpu.VMEM((ROWS, 2 * HEAD), BF16),
            pltpu.VMEM((448, 8, ROWS), F32),
            pltpu.SMEM((128,), jnp.int32),
            pltpu.SemaphoreType.DMA((7,)),
            pltpu.SemaphoreType.DMA((4,)),
            pltpu.SemaphoreType.DMA((52,)),
        ],
        compiler_params=pltpu.CompilerParams(collective_id=0, has_side_effects=True, vmem_limit_bytes=24 * 1024 * 1024),
        name="attention",
    )(*[pltpu.with_memory_space_constraint(a, pltpu.HBM) for a in (queries, keys, values, block_order)])
    return pl.pallas_call(
        settle,
        out_shape=(
            jax.ShapeDtypeStruct((32, 4096), BF16),
            jax.ShapeDtypeStruct((4, ROWS), F32),
        ),
        in_specs=[vmem, vmem],
        out_specs=(hbm, hbm),
        scratch_shapes=[pltpu.SemaphoreType.DMA((2,))],
        compiler_params=pltpu.CompilerParams(vmem_limit_bytes=2 * 1024 * 1024),
        name="settle",
    )(*results)


def solution(mesh):
    in_specs = (P("seq", "head"), P("seq", "head"), P("seq", "head"), P())
    out_specs = (P(("seq", "head"), None), P("head", "seq"))
    return jax.shard_map(local, mesh=mesh, in_specs=in_specs, out_specs=out_specs, check_vma=False)
```

```python
import functools

import jax
import jax.numpy as jnp
from jax import lax
from jax.experimental import pallas as pl
from jax.experimental.pallas import tpu as pltpu
from jax.sharding import PartitionSpec as P

MESH = pl.DeviceIdType.MESH
HEAD = 256
ROWS = 128
BLK = 64
NZ, NY = 8, 4
NEG = -1e30
BIG = 1e30
SCALE = 1.4426950408889634 / 16.0
FLOOR = -1e6
LN2 = 0.6931471805599453
F32 = jnp.float32
BF16 = jnp.bfloat16

RIGHT_SLOTS = (0, 1, 2, 3, 7)
LEFT_SLOTS = (0, 4, 5, 6, 7)
SLOT_DZ = (0, -1, -2, -3, 1, 2, 3, 4)
QUERY_DY = (0, -1, 1, 2)


def combine(parts):
    top = functools.reduce(jnp.maximum, [lse for _, lse in parts])
    weights = [jnp.exp2(lse - top) for _, lse in parts]
    total = functools.reduce(jnp.add, weights)
    scale = 1.0 / total
    out = functools.reduce(jnp.add, [o.astype(F32) * (w * scale) for (o, _), w in zip(parts, weights)])
    return out, top + jnp.log2(total)


def kernel(q_ref, k_ref, v_ref, order_hbm, attn_ref, lse_ref,
           qbuf, kbuf, vbuf, vm, vsw, qpos, acc, mx, ls,
           osend, lsend, orecv, lrecv, obuf, abuf, lxs, lxr, sa, sb, pa, pb, km, qm, yard, order_ref,
           local_sem, send_sem, recv_sem):
    s = lax.axis_index("seq")
    g = lax.axis_index("head")
    z = s // (2 * NY)
    y = (s // 2) % NY
    c = s % 2

    def at(dz, dy):
        return (((z + dz + NZ) % NZ) * NY + (y + dy + NY) % NY) * 2 + c

    partner = (s + 1 - 2 * c, g)
    up, down = (at(1, 0), g), (at(-1, 0), g)
    fore, back = (at(0, 1), g), (at(0, -1), g)

    loads = [
        pltpu.make_async_copy(v_ref, vm, local_sem.at[0]),
        pltpu.make_async_copy(k_ref.at[:, pl.ds(pl.multiple_of(c * HEAD, HEAD), HEAD)], kbuf.at[0, pl.ds(0, ROWS), :], local_sem.at[1]),
    ]
    for hd in range(2):
        loads.append(pltpu.make_async_copy(
            q_ref.at[:, pl.ds(pl.multiple_of(c * 2 * HEAD + hd * HEAD, HEAD), HEAD)],
            qbuf.at[0, pl.ds(hd * ROWS, ROWS), :], local_sem.at[2 + hd]))
    loads += [
        pltpu.make_async_copy(k_ref.at[:, pl.ds(pl.multiple_of((1 - c) * HEAD, HEAD), HEAD)], km, local_sem.at[4]),
        pltpu.make_async_copy(q_ref.at[:, pl.ds(pl.multiple_of((1 - c) * 2 * HEAD, HEAD), 2 * HEAD)], qm, local_sem.at[5]),
    ]
    order_load = pltpu.make_async_copy(order_hbm, order_ref, local_sem.at[6])
    for n in (1, 4, 2, 3, 0, 5):
        loads[n].start()
    order_load.start()

    line = []
    for r in range(2):
        for e in range(4):
            if r or e:
                line.append(((s if r == 0 else s + 1 - 2 * c), (g + e) % 4))
    barrier = pltpu.get_barrier_semaphore()
    for peer in line + [up, down, fore, back]:
        pl.semaphore_signal(barrier, inc=1, device_id=peer, device_id_type=MESH)

    table = {}
    recv_slots = {}

    def recv_slot(key):
        return recv_sem.at[recv_slots.setdefault(key, len(recv_slots))]

    def message(name, src, dst, device, group, key=None):
        table[name] = pltpu.make_async_remote_copy(
            src_ref=src, dst_ref=dst, send_sem=send_sem.at[group], recv_sem=recv_slot(name if key is None else key),
            device_id=device, device_id_type=MESH)

    def drain(sem, kib):
        ref = yard.at[pl.ds(0, kib // 4)]
        pltpu.make_async_copy(ref, ref, sem).wait()

    other = 1 - c
    for hd in range(2):
        message(("xq", hd), qm.at[:, pl.ds(hd * HEAD, HEAD)], qbuf.at[4, pl.ds(hd * ROWS, ROWS), :], partner, 1)
    message("xk", km, kbuf.at[0, pl.ds(ROWS, ROWS), :], partner, 1)
    message("xv", vsw, vbuf.at[0, :, pl.ds(ROWS, ROWS)], partner, 1)
    for h in range(2):
        def kpart(slot):
            return kbuf.at[slot, pl.ds(h * ROWS, ROWS), :]

        def vpart(slot):
            return vbuf.at[slot, :, pl.ds(h * ROWS, ROWS)]

        for t in range(1, 5):
            key = ("end", h) if t == 4 else None
            message(("rk", h, t), kpart(RIGHT_SLOTS[t - 1]), kpart(RIGHT_SLOTS[t]), up, 0, key)
            message(("lv", h, t), vpart(LEFT_SLOTS[t - 1]), vpart(LEFT_SLOTS[t]), down, 0, key)
            if t < 4:
                message(("lk", h, t), kpart(LEFT_SLOTS[t - 1]), kpart(LEFT_SLOTS[t]), down, 0)
                message(("rv", h, t), vpart(RIGHT_SLOTS[t - 1]), vpart(RIGHT_SLOTS[t]), up, 0)

        def qpart(slot, hd):
            return qbuf.at[h * 4 + slot, pl.ds(hd * ROWS, ROWS), :]

        message(("qr", h, 0), qpart(0, 0), qpart(1, 0), fore, 1)
        message(("ql", h, 1), qpart(0, 1), qpart(2, 1), back, 1)
        message(("qr", h, 1), qpart(0, 1), qpart(1, 1), fore, 1, ("near", h))
        message(("ql", h, 0), qpart(0, 0), qpart(2, 0), back, 1, ("near", h))
        message(("qrr", h), qpart(1, 0), qpart(3, 0), fore, 1, ("far", h))
        message(("qll", h), qpart(2, 1), qpart(3, 1), back, 1, ("far", h))
    for n in range(6):
        device = fore if n % 2 == 0 else back
        for hd in range(2):
            message(("l", n, hd), lsend.at[2 * n + hd], lrecv.at[2 * n + hd], device, 3, ("taken", n, hd))
            message(("o", n, hd), osend.at[2 * n + hd], orecv.at[2 * n + hd], device, 2, ("taken", n, hd))
    for hd in range(2):
        message(("lx", hd), lxs.at[hd], lxr.at[hd], partner, 3, "lx")
    for r in range(2):
        for e in range(4):
            for hd in range(2):
                if r or e:
                    rows = pl.ds(pl.multiple_of(((g + e) % 4) * 32, 32), 32)
                    cols = pl.ds(pl.multiple_of(((2 * g + c) * 2 + hd) * HEAD, HEAD), HEAD)
                    there = s if r == 0 else s + 1 - 2 * c
                    message(("line", r, e, hd), obuf.at[r, rows, pl.ds(hd * HEAD, HEAD)], abuf.at[:, cols],
                            (there, (g + e) % 4), 3, "line")

    def send(name):
        table[name].start()

    def arrive(name):
        table[name].wait_recv()

    def key_bases(slot):
        out = []
        for h in range(2):
            origin = (((z + SLOT_DZ[slot] + NZ) % NZ) * NY + y) * 2 + (c if h == 0 else other)
            out += [order_ref[2 * origin] * BLK, order_ref[2 * origin + 1] * BLK]
        return out

    iota = lax.broadcasted_iota(jnp.int32, (BLK, HEAD), 0)

    score_buffers, weight_buffers = (sa, sb), (pa, pb)
    bases_of = {}
    queue = []
    count = [0]

    def stage_scores(item):
        i, slots = item["tile"], item["slots"]
        into = score_buffers[item["turn"] % 2]
        q = qbuf[i]
        for n, slot in enumerate(slots):
            into[n * 256:(n + 1) * 256, :] = lax.dot_general(
                kbuf[slot], q, (((1,), (1,)), ((), ())), preferred_element_type=F32)

    def stage_weights(item):
        i, slots = item["tile"], item["slots"]
        source, into = score_buffers[item["turn"] % 2], weight_buffers[item["turn"] % 2]
        diagonal = slots == (0,) and i in (0, 4)
        first = slots == (0,)
        position = qpos[i, 0:1, :]
        for slot in slots:
            if slot not in bases_of:
                bases_of[slot] = key_bases(slot)
        bases = [base for slot in slots for base in bases_of[slot]]

        def raw(b):
            block = source[b * BLK:(b + 1) * BLK, :]
            return jnp.where(iota <= position - bases[b], block, NEG) if diagonal else block

        old = jnp.full((1, HEAD), FLOOR, F32) if first else mx[i, 0:1, :]
        allowed = [base <= position for base in bases]
        best = functools.reduce(jnp.maximum, [
            jnp.where(allowed[b], jnp.max(raw(b).reshape(8, 8, HEAD), axis=0), NEG) for b in range(len(bases))])
        best = jnp.max(best, axis=0, keepdims=True) * SCALE
        fresh = jnp.maximum(old, best)
        sums = None
        for b in range(len(bases)):
            weights = jnp.exp2(raw(b) * SCALE - jnp.where(allowed[b], fresh, BIG))
            part = jnp.sum(weights.reshape(8, 8, HEAD), axis=0)
            sums = part if sums is None else sums + part
            into[b * BLK:(b + 1) * BLK, :] = weights.astype(BF16)
        if first:
            item["factor"] = None
        else:
            item["factor"] = jnp.exp2(old - fresh)
            sums = ls[i] * item["factor"] + sums
        if item["last"]:
            item["top"], item["sums"] = fresh, sums
        else:
            mx[i] = jnp.broadcast_to(fresh, (8, HEAD))
            ls[i] = sums

    def stage_values(item):
        i, slots = item["tile"], item["slots"]
        source = weight_buffers[item["turn"] % 2]
        update = functools.reduce(jnp.add, [
            lax.dot_general(vbuf[slot], source[n * 256:(n + 1) * 256, :], (((1,), (0,)), ((), ())), preferred_element_type=F32)
            for n, slot in enumerate(slots)
        ])
        if item["factor"] is not None:
            update = acc[i] * item["factor"] + update
        if item["last"]:
            l = jnp.sum(item["sums"], axis=0, keepdims=True)
            some = l > 0.0
            inverse = jnp.where(some, 1.0 / jnp.where(some, l, 1.0), 0.0)
            item["done"](update * inverse, jnp.where(some, item["top"] + jnp.log2(jnp.where(some, l, 1.0)), NEG))
        else:
            acc[i] = update

    def advance():
        if queue and queue[-1]["stage"] == 0:
            stage_scores(queue[-1])
        for item in queue[::-1]:
            if item["stage"] == 1:
                stage_weights(item)
            elif item["stage"] == 2:
                stage_values(item)
        for item in queue:
            item["stage"] += 1
        queue[:] = [item for item in queue if item["stage"] < 3]

    def push(tiles, slots, done=None):
        for i in tiles:
            queue.append({"tile": i, "slots": slots, "turn": count[0], "stage": 0, "last": done is not None, "done": done})
            count[0] += 1
            advance()

    def flush():
        while queue:
            advance()

    def first_hop(kind, h):
        send(("r" + kind, h, 1))
        send(("l" + kind, h, 1))

    def ring_keys(h, t):
        arrive(("rk", h, t))
        if (h, t) != (0, 3):
            send(("rk", h, t + 1))
        arrive(("lk", h, t))
        if t < 3:
            send(("lk", h, t + 1))

    def ring_values(h, t):
        arrive(("lv", h, t))
        if (h, t) != (0, 3):
            send(("lv", h, t + 1))
        arrive(("rv", h, t))
        if t < 3:
            send(("rv", h, t + 1))

    def ring_end(h):
        drain(recv_slot(("end", h)), 128)

    def spread(hd):
        arrive(("xq", hd))
        send(("qr", 1, hd))
        send(("ql", 1, hd))

    def relay(h):
        arrive(("qr", h, 0))
        send(("qrr", h))
        arrive(("ql", h, 1))
        send(("qll", h))
        drain(recv_slot(("near", h)), 128)

    def relayed(h):
        drain(recv_slot(("far", h)), 128)

    def cross_values():
        arrive("xv")
        first_hop("v", 1)

    def cross_keys():
        arrive("xk")
        first_hop("k", 1)

    assert len(recv_slots) == 52, len(recv_slots)
    loads[1].wait()
    loads[4].wait()
    pl.semaphore_wait(barrier, 11)
    first_hop("k", 0)
    send("xk")
    for hd in range(2):
        loads[2 + hd].wait()
        send(("qr", 0, hd))
        send(("ql", 0, hd))

    def flipped(column):
        v = vm[:, pl.ds(pl.multiple_of(column * HEAD, HEAD), HEAD)]
        return v.astype(F32).T.astype(BF16)

    loads[0].wait()
    vbuf[0, :, 0:ROWS] = flipped(c)
    vsw[...] = flipped(other)
    order_load.wait()
    lane = lax.broadcasted_iota(jnp.int32, (8, HEAD), 1)
    for slot in range(4):
        for h in range(2):
            origin = (z * NY + (y + QUERY_DY[slot] + NY) % NY) * 2 + (c if h == 0 else other)
            first, second = order_ref[2 * origin] * BLK, order_ref[2 * origin + 1] * BLK
            inside = lane % ROWS
            qpos[h * 4 + slot] = jnp.where(inside < BLK, first + inside, second + inside - BLK)
    send("xv")
    first_hop("v", 0)
    loads[5].wait()
    send(("xq", 0))
    send(("xq", 1))

    ring_keys(0, 1)
    cross_keys()
    relay(0)
    ring_values(0, 1)
    cross_values()
    push((0, 1, 2), (0,))
    spread(0)
    spread(1)
    ring_keys(0, 2)
    relayed(0)
    push((3,), (0,))
    ring_keys(1, 1)
    push((4,), (0,))
    ring_values(0, 2)
    ring_values(1, 1)
    push((0, 1), (1, 4))
    relay(1)
    push((2, 3), (1, 4))
    ring_keys(0, 3)
    push((5, 6), (0,))
    push((4, 5), (1, 4))
    ring_keys(1, 2)
    ring_values(0, 3)
    push((6,), (1, 4))
    ring_values(1, 2)
    send(("rk", 0, 4))
    send(("lv", 0, 4))
    relayed(1)
    push((7,), (0,))
    push((7,), (1, 4))
    push((0, 1), (2, 5))
    ring_keys(1, 3)
    push((2, 3, 4), (2, 5))
    ring_values(1, 3)
    push((5, 6, 7), (2, 5))
    push((0, 1, 2, 3, 4, 5, 6, 7), (3, 6))
    ring_end(0)
    ring_end(1)

    def piece(i, hd):
        return acc[i, :, hd * ROWS:(hd + 1) * ROWS], mx[i, 0:1, hd * ROWS:(hd + 1) * ROWS]

    def stage_out(n, hd, o, lse):
        osend[2 * n + hd] = o.astype(BF16)
        lsend[2 * n + hd] = jnp.broadcast_to(lse, (8, ROWS))

    def ship(n, hd):
        send(("l", n, hd))
        send(("o", n, hd))

    def taken(n, hd):
        drain(recv_slot(("taken", n, hd)), 68)
        return orecv[2 * n + hd], lrecv[2 * n + hd, 0:1, :]

    direct = {3: 0, 7: 1, 6: 2, 1: 3}

    def done_with(tile):
        def done(o, lse):
            if tile in direct:
                n = direct[tile]
                for hd in range(2):
                    stage_out(n, hd, o[:, hd * ROWS:(hd + 1) * ROWS], lse[:, hd * ROWS:(hd + 1) * ROWS])
                    if n < 2 or hd == 0:
                        ship(n, hd)
            else:
                acc[tile] = o
                mx[tile] = jnp.broadcast_to(lse, (8, HEAD))
        return done

    for tile in (3, 7, 6, 1, 2, 5, 0, 4):
        push((tile,), (7,), done_with(tile))
    flush()
    for hd in range(2):
        for n, tile in ((0, 2), (1, 5)):
            stage_out(4 + n, hd, *combine([piece(tile, hd), taken(n, hd)]))
            ship(4 + n, hd)
            if hd == 0:
                ship(2 + n, 1)

    def result(r, hd):
        pieces = [piece(0, hd), taken(3, hd), taken(4, hd)] if r == 0 else [piece(4, hd), taken(2, hd), taken(5, hd)]
        out, lse = combine(pieces)
        lse = lse * LN2
        if r:
            lxs[hd] = jnp.broadcast_to(lse, (8, ROWS))
            send(("lx", hd))
        else:
            lse_ref[pl.ds(2 * c + hd, 1), :] = lse
        obuf[r, :, hd * HEAD:(hd + 1) * HEAD] = out.T.astype(BF16)
        for e in range(4):
            if r or e:
                send(("line", r, e, hd))

    for hd in range(2):
        result(1, hd)
        result(0, hd)
    cols = pl.ds(pl.multiple_of((2 * g + c) * 2 * HEAD, 2 * HEAD), 2 * HEAD)
    abuf[:, cols] = obuf[0, pl.ds(pl.multiple_of(g * 32, 32), 32), :]
    drain(recv_slot("lx"), 8)
    for hd in range(2):
        lse_ref[pl.ds(2 * other + hd, 1), :] = lxr[hd, 0:1, :]
    drain(recv_slot("line"), 224)
    attn_ref[...] = abuf[...]
    for group, kib in enumerate((28 * 64, 16 * 64, 12 * 64, 280)):
        drain(send_sem.at[group], kib)


def settle(attn_in, lse_in, attn_out, lse_out, sem):
    copies = [
        pltpu.make_async_copy(attn_in, attn_out, sem.at[0]),
        pltpu.make_async_copy(lse_in, lse_out, sem.at[1]),
    ]
    for copy in copies:
        copy.start()
    for copy in copies:
        copy.wait()


def local(queries, keys, values, block_order):
    hbm = pl.BlockSpec(memory_space=pltpu.HBM)
    vmem = pl.BlockSpec(memory_space=pltpu.VMEM)
    results = pl.pallas_call(
        kernel,
        out_shape=(
            jax.ShapeDtypeStruct((32, 4096), BF16),
            jax.ShapeDtypeStruct((4, ROWS), F32),
        ),
        in_specs=[hbm, hbm, hbm, hbm],
        out_specs=(vmem, vmem),
        scratch_shapes=[
            pltpu.VMEM((8, 256, HEAD), BF16),
            pltpu.VMEM((8, 256, HEAD), BF16),
            pltpu.VMEM((8, HEAD, 256), BF16),
            pltpu.VMEM((ROWS, 2 * HEAD), BF16),
            pltpu.VMEM((HEAD, ROWS), BF16),
            pltpu.VMEM((8, 8, HEAD), jnp.int32),
            pltpu.VMEM((8, HEAD, 256), F32),
            pltpu.VMEM((8, 8, 256), F32),
            pltpu.VMEM((8, 8, 256), F32),
            pltpu.VMEM((12, HEAD, ROWS), BF16),
            pltpu.VMEM((12, 8, ROWS), F32),
            pltpu.VMEM((12, HEAD, ROWS), BF16),
            pltpu.VMEM((12, 8, ROWS), F32),
            pltpu.VMEM((2, ROWS, 2 * HEAD), BF16),
            pltpu.VMEM((32, 4096), BF16),
            pltpu.VMEM((2, 8, ROWS), F32),
            pltpu.VMEM((2, 8, ROWS), F32),
            pltpu.VMEM((512, HEAD), F32),
            pltpu.VMEM((512, HEAD), F32),
            pltpu.VMEM((512, HEAD), BF16),
            pltpu.VMEM((512, HEAD), BF16),
            pltpu.VMEM((ROWS, HEAD), BF16),
            pltpu.VMEM((ROWS, 2 * HEAD), BF16),
            pltpu.VMEM((448, 8, ROWS), F32),
            pltpu.SMEM((128,), jnp.int32),
            pltpu.SemaphoreType.DMA((7,)),
            pltpu.SemaphoreType.DMA((4,)),
            pltpu.SemaphoreType.DMA((52,)),
        ],
        compiler_params=pltpu.CompilerParams(collective_id=0, has_side_effects=True, vmem_limit_bytes=24 * 1024 * 1024),
        name="attention",
    )(*[pltpu.with_memory_space_constraint(a, pltpu.HBM) for a in (queries, keys, values, block_order)])
    return pl.pallas_call(
        settle,
        out_shape=(
            jax.ShapeDtypeStruct((32, 4096), BF16),
            jax.ShapeDtypeStruct((4, ROWS), F32),
        ),
        in_specs=[vmem, vmem],
        out_specs=(hbm, hbm),
        scratch_shapes=[pltpu.SemaphoreType.DMA((2,))],
        compiler_params=pltpu.CompilerParams(vmem_limit_bytes=2 * 1024 * 1024),
        name="settle",
    )(*results)


def solution(mesh):
    in_specs = (P("seq", "head"), P("seq", "head"), P("seq", "head"), P())
    out_specs = (P(("seq", "head"), None), P("head", "seq"))
    return jax.shard_map(local, mesh=mesh, in_specs=in_specs, out_specs=out_specs, check_vma=False)
```

```python
import functools

import jax
import jax.numpy as jnp
from jax import lax
from jax.experimental import pallas as pl
from jax.experimental.pallas import tpu as pltpu
from jax.sharding import PartitionSpec as P

MESH = pl.DeviceIdType.MESH
HEAD = 256
ROWS = 128
BLK = 64
NZ, NY = 8, 4
NEG = -1e30
BIG = 1e30
SCALE = 1.4426950408889634 / 16.0
FLOOR = -1e6
LN2 = 0.6931471805599453
F32 = jnp.float32
BF16 = jnp.bfloat16

RIGHT_SLOTS = (0, 1, 2, 3, 7)
LEFT_SLOTS = (0, 4, 5, 6, 7)
SLOT_DZ = (0, -1, -2, -3, 1, 2, 3, 4)
QUERY_DY = (0, -1, 1, 2)


def log_total(rows):
    top = functools.reduce(jnp.maximum, rows)
    return top + jnp.log2(functools.reduce(jnp.add, [jnp.exp2(row - top) for row in rows]))


def kernel(q_ref, k_ref, v_ref, order_hbm, attn_ref, lse_ref,
           qbuf, kbuf, vbuf, vm, vsw, qpos, acc, mx, ls,
           osend, lstat, orecv, lgot, cbuf, abufc, obuf, abuf, lxs, lxr, sa, sb, pa, pb, km, qm, yard, order_ref,
           local_sem, send_sem, recv_sem):
    s = lax.axis_index("seq")
    g = lax.axis_index("head")
    z = s // (2 * NY)
    y = (s // 2) % NY
    c = s % 2

    def at(dz, dy):
        return (((z + dz + NZ) % NZ) * NY + (y + dy + NY) % NY) * 2 + c

    partner = (s + 1 - 2 * c, g)
    up, down = (at(1, 0), g), (at(-1, 0), g)
    fore, back = (at(0, 1), g), (at(0, -1), g)

    loads = [
        pltpu.make_async_copy(v_ref, vm, local_sem.at[0]),
        pltpu.make_async_copy(k_ref.at[:, pl.ds(pl.multiple_of(c * HEAD, HEAD), HEAD)], kbuf.at[0, pl.ds(0, ROWS), :], local_sem.at[1]),
    ]
    for hd in range(2):
        loads.append(pltpu.make_async_copy(
            q_ref.at[:, pl.ds(pl.multiple_of(c * 2 * HEAD + hd * HEAD, HEAD), HEAD)],
            qbuf.at[0, pl.ds(hd * ROWS, ROWS), :], local_sem.at[2 + hd]))
    loads += [
        pltpu.make_async_copy(k_ref.at[:, pl.ds(pl.multiple_of((1 - c) * HEAD, HEAD), HEAD)], km, local_sem.at[4]),
        pltpu.make_async_copy(q_ref.at[:, pl.ds(pl.multiple_of((1 - c) * 2 * HEAD, HEAD), 2 * HEAD)], qm, local_sem.at[5]),
    ]
    order_load = pltpu.make_async_copy(order_hbm, order_ref, local_sem.at[6])
    for n in (1, 4, 2, 3, 0, 5):
        loads[n].start()
    order_load.start()

    def across(index):
        return index + 1 - 2 * c

    far = (at(0, 2), g)
    peers = [up, down, fore, back]
    for e in range(4):
        peers.append((across(s), (g + e) % 4))
        if e:
            peers.append((s, (g + e) % 4))
    barrier = pltpu.get_barrier_semaphore()
    for peer in peers:
        pl.semaphore_signal(barrier, inc=1, device_id=peer, device_id_type=MESH)

    table = {}
    recv_slots = {}

    def recv_slot(key):
        return recv_sem.at[recv_slots.setdefault(key, len(recv_slots))]

    def message(name, src, dst, device, group, key=None):
        table[name] = pltpu.make_async_remote_copy(
            src_ref=src, dst_ref=dst, send_sem=send_sem.at[group], recv_sem=recv_slot(name if key is None else key),
            device_id=device, device_id_type=MESH)

    def drain(sem, kib):
        ref = yard.at[pl.ds(0, kib // 4)]
        pltpu.make_async_copy(ref, ref, sem).wait()

    other = 1 - c
    for hd in range(2):
        message(("xq", hd), qm.at[:, pl.ds(hd * HEAD, HEAD)], qbuf.at[4, pl.ds(hd * ROWS, ROWS), :], partner, 1)
    message("xk", km, kbuf.at[0, pl.ds(ROWS, ROWS), :], partner, 1)
    message("xv", vsw, vbuf.at[0, :, pl.ds(ROWS, ROWS)], partner, 1)
    for h in range(2):
        def kpart(slot):
            return kbuf.at[slot, pl.ds(h * ROWS, ROWS), :]

        def vpart(slot):
            return vbuf.at[slot, :, pl.ds(h * ROWS, ROWS)]

        for t in range(1, 5):
            key = ("end", h) if t == 4 else None
            message(("rk", h, t), kpart(RIGHT_SLOTS[t - 1]), kpart(RIGHT_SLOTS[t]), up, 0, key)
            message(("lv", h, t), vpart(LEFT_SLOTS[t - 1]), vpart(LEFT_SLOTS[t]), down, 0, key)
            if t < 4:
                message(("lk", h, t), kpart(LEFT_SLOTS[t - 1]), kpart(LEFT_SLOTS[t]), down, 0)
                message(("rv", h, t), vpart(RIGHT_SLOTS[t - 1]), vpart(RIGHT_SLOTS[t]), up, 0)

        def qpart(slot, hd):
            return qbuf.at[h * 4 + slot, pl.ds(hd * ROWS, ROWS), :]

        message(("qr", h, 0), qpart(0, 0), qpart(1, 0), fore, 1)
        message(("ql", h, 1), qpart(0, 1), qpart(2, 1), back, 1)
        message(("qr", h, 1), qpart(0, 1), qpart(1, 1), fore, 1, ("near", h))
        message(("ql", h, 0), qpart(0, 0), qpart(2, 0), back, 1, ("near", h))
        message(("qrr", h), qpart(1, 0), qpart(3, 0), fore, 1, ("far", h))
        message(("qll", h), qpart(2, 1), qpart(3, 1), back, 1, ("far", h))
    for n in range(4):
        for hd in range(2):
            message(("o", n, hd), osend.at[2 * n + hd], orecv.at[2 * n + hd], fore if n % 2 == 0 else back, 2)
    for n, device in enumerate((fore, back, far)):
        message(("stat", n), lstat, lgot.at[n], device, 3, "stat")
    for hd in range(2):
        message(("lx", hd), lxs.at[hd], lxr.at[hd], partner, 3, "lx")
    for hd in range(2):
        cols = pl.ds(pl.multiple_of(((2 * g + c) * 2 + hd) * HEAD, HEAD), HEAD)
        half_cols = pl.ds(hd * HEAD, HEAD)
        for e in range(4):
            there = (g + e) % 4
            rows = pl.ds(pl.multiple_of(there * 32, 32), 32)
            for n, target in enumerate((at(0, 1), across(at(0, -1)))):
                message(("side", n, e, hd), cbuf.at[n, rows, half_cols], abufc.at[:, cols], (target, there), 2, "side")
            for r, target in enumerate((s, across(s))):
                if r or e:
                    message(("line", r, e, hd), obuf.at[r, rows, half_cols], abuf.at[:, cols], (target, there), 3, "line")

    def send(name):
        table[name].start()

    def arrive(name):
        table[name].wait_recv()

    def key_bases(slot):
        out = []
        for h in range(2):
            origin = (((z + SLOT_DZ[slot] + NZ) % NZ) * NY + y) * 2 + (c if h == 0 else other)
            out += [order_ref[2 * origin] * BLK, order_ref[2 * origin + 1] * BLK]
        return out

    iota = lax.broadcasted_iota(jnp.int32, (BLK, HEAD), 0)

    score_buffers, weight_buffers = (sa, sb), (pa, pb)
    bases_of = {}
    queue = []
    count = [0]

    def stage_scores(item):
        i, slots = item["tile"], item["slots"]
        into = score_buffers[item["turn"] % 2]
        q = qbuf[i]
        for n, slot in enumerate(slots):
            into[n * 256:(n + 1) * 256, :] = lax.dot_general(
                kbuf[slot], q, (((1,), (1,)), ((), ())), preferred_element_type=F32)

    def stage_weights(item):
        i, slots = item["tile"], item["slots"]
        source, into = score_buffers[item["turn"] % 2], weight_buffers[item["turn"] % 2]
        diagonal = slots == (0,) and i in (0, 4)
        first = slots == (0,)
        position = qpos[i, 0:1, :]
        for slot in slots:
            if slot not in bases_of:
                bases_of[slot] = key_bases(slot)
        bases = [base for slot in slots for base in bases_of[slot]]

        def raw(b):
            block = source[b * BLK:(b + 1) * BLK, :]
            return jnp.where(iota <= position - bases[b], block, NEG) if diagonal else block

        old = jnp.full((1, HEAD), FLOOR, F32) if first else mx[i, 0:1, :]
        allowed = [base <= position for base in bases]
        best = functools.reduce(jnp.maximum, [
            jnp.where(allowed[b], jnp.max(raw(b).reshape(8, 8, HEAD), axis=0), NEG) for b in range(len(bases))])
        best = jnp.max(best, axis=0, keepdims=True) * SCALE
        fresh = jnp.maximum(old, best)
        sums = None
        for b in range(len(bases)):
            weights = jnp.exp2(raw(b) * SCALE - jnp.where(allowed[b], fresh, BIG))
            part = jnp.sum(weights.reshape(8, 8, HEAD), axis=0)
            sums = part if sums is None else sums + part
            into[b * BLK:(b + 1) * BLK, :] = weights.astype(BF16)
        if first:
            item["factor"] = None
        else:
            item["factor"] = jnp.exp2(old - fresh)
            sums = ls[i] * item["factor"] + sums
        if item["last"]:
            item["top"], item["sums"] = fresh, sums
        else:
            mx[i] = jnp.broadcast_to(fresh, (8, HEAD))
            ls[i] = sums

    def stage_values(item):
        i, slots = item["tile"], item["slots"]
        source = weight_buffers[item["turn"] % 2]
        update = functools.reduce(jnp.add, [
            lax.dot_general(vbuf[slot], source[n * 256:(n + 1) * 256, :], (((1,), (0,)), ((), ())), preferred_element_type=F32)
            for n, slot in enumerate(slots)
        ])
        if item["factor"] is not None:
            update = acc[i] * item["factor"] + update
        if item["last"]:
            l = jnp.sum(item["sums"], axis=0, keepdims=True)
            some = l > 0.0
            inverse = jnp.where(some, 1.0 / jnp.where(some, l, 1.0), 0.0)
            item["done"](update * inverse, jnp.where(some, item["top"] + jnp.log2(jnp.where(some, l, 1.0)), NEG))
        else:
            acc[i] = update

    def advance():
        if queue and queue[-1]["stage"] == 0:
            stage_scores(queue[-1])
        for item in queue[::-1]:
            if item["stage"] == 1:
                stage_weights(item)
            elif item["stage"] == 2:
                stage_values(item)
        for item in queue:
            item["stage"] += 1
        queue[:] = [item for item in queue if item["stage"] < 3]

    def push(tiles, slots, done=None):
        for i in tiles:
            queue.append({"tile": i, "slots": slots, "turn": count[0], "stage": 0, "last": done is not None, "done": done})
            count[0] += 1
            advance()

    def flush():
        while queue:
            advance()

    def first_hop(kind, h):
        send(("r" + kind, h, 1))
        send(("l" + kind, h, 1))

    def ring_keys(h, t):
        arrive(("rk", h, t))
        if (h, t) != (0, 3):
            send(("rk", h, t + 1))
        arrive(("lk", h, t))
        if t < 3:
            send(("lk", h, t + 1))

    def ring_values(h, t):
        arrive(("lv", h, t))
        if (h, t) != (0, 3):
            send(("lv", h, t + 1))
        arrive(("rv", h, t))
        if t < 3:
            send(("rv", h, t + 1))

    def ring_end(h):
        drain(recv_slot(("end", h)), 128)

    def spread(hd):
        arrive(("xq", hd))
        send(("qr", 1, hd))
        send(("ql", 1, hd))

    def relay(h):
        arrive(("qr", h, 0))
        send(("qrr", h))
        arrive(("ql", h, 1))
        send(("qll", h))
        drain(recv_slot(("near", h)), 128)

    def relayed(h):
        drain(recv_slot(("far", h)), 128)

    def cross_values():
        arrive("xv")
        first_hop("v", 1)

    def cross_keys():
        arrive("xk")
        first_hop("k", 1)

    assert len(recv_slots) == 50, len(recv_slots)
    loads[1].wait()
    loads[4].wait()
    pl.semaphore_wait(barrier, len(peers))
    first_hop("k", 0)
    send("xk")
    for hd in range(2):
        loads[2 + hd].wait()
        send(("qr", 0, hd))
        send(("ql", 0, hd))

    def flipped(column):
        v = vm[:, pl.ds(pl.multiple_of(column * HEAD, HEAD), HEAD)]
        return v.astype(F32).T.astype(BF16)

    loads[0].wait()
    vbuf[0, :, 0:ROWS] = flipped(c)
    vsw[...] = flipped(other)
    order_load.wait()
    lane = lax.broadcasted_iota(jnp.int32, (8, HEAD), 1)
    for slot in range(4):
        for h in range(2):
            origin = (z * NY + (y + QUERY_DY[slot] + NY) % NY) * 2 + (c if h == 0 else other)
            first, second = order_ref[2 * origin] * BLK, order_ref[2 * origin + 1] * BLK
            inside = lane % ROWS
            qpos[h * 4 + slot] = jnp.where(inside < BLK, first + inside, second + inside - BLK)
    send("xv")
    first_hop("v", 0)
    loads[5].wait()
    send(("xq", 0))
    send(("xq", 1))

    ring_keys(0, 1)
    cross_keys()
    relay(0)
    ring_values(0, 1)
    cross_values()
    push((0, 1, 2), (0,))
    spread(0)
    spread(1)
    ring_keys(0, 2)
    relayed(0)
    push((3,), (0,))
    ring_keys(1, 1)
    push((4,), (0,))
    ring_values(0, 2)
    ring_values(1, 1)
    push((0, 1), (1, 4))
    relay(1)
    push((2, 3), (1, 4))
    ring_keys(0, 3)
    push((5, 6), (0,))
    push((4, 5), (1, 4))
    ring_keys(1, 2)
    ring_values(0, 3)
    push((6,), (1, 4))
    ring_values(1, 2)
    send(("rk", 0, 4))
    send(("lv", 0, 4))
    relayed(1)
    push((7,), (0,))
    push((7,), (1, 4))
    push((0, 1), (2, 5))
    ring_keys(1, 3)
    push((2, 3, 4), (2, 5))
    ring_values(1, 3)
    push((5, 6, 7), (2, 5))
    push((0, 1, 2, 3, 4, 5, 6, 7), (3, 6))
    ring_end(0)
    ring_end(1)

    def half(hd):
        return slice(hd * ROWS, (hd + 1) * ROWS)

    direct = {3: 0, 7: 1, 6: 2, 1: 3}

    def done_with(tile):
        def done(o, lse):
            lstat[tile:tile + 1, :] = lse
            if tile in direct:
                n = direct[tile]
                for hd in range(2):
                    osend[2 * n + hd] = o[:, half(hd)].astype(BF16)
                    if n < 2 and hd == 0:
                        send(("o", n, hd))
            else:
                acc[tile] = o
        return done

    for tile in (3, 7, 6, 1, 2, 5, 0, 4):
        push((tile,), (7,), done_with(tile))
    flush()
    for n in range(3):
        send(("stat", n))
    for n, hd in ((0, 1), (1, 1), (2, 0), (3, 0), (2, 1), (3, 1)):
        send(("o", n, hd))
    drain(recv_slot("stat"), 24)

    def mine(i):
        return lstat[i:i + 1, :]

    def theirs(n, i):
        return lgot[n, i:i + 1, :]

    side_total = [
        log_total([mine(2), theirs(0, 3), theirs(1, 0), theirs(2, 1)]),
        log_total([mine(5), theirs(1, 7), theirs(0, 4), theirs(2, 6)]),
    ]
    own_total = [log_total([mine(4 * h), theirs(0, 4 * h + 2), theirs(1, 4 * h + 1), theirs(2, 4 * h + 3)]) for h in range(2)]
    for hd in range(2):
        lxs[hd] = jnp.broadcast_to(own_total[1][:, half(hd)] * LN2, (8, ROWS))
        send(("lx", hd))
        lse_ref[pl.ds(2 * c + hd, 1), :] = own_total[0][:, half(hd)] * LN2

    def joined(tile, n, hd, total, lse):
        arrive(("o", n, hd))
        out = acc[tile, :, half(hd)] * jnp.exp2(mine(tile) - total)[:, half(hd)]
        out = out + orecv[2 * n + hd].astype(F32) * jnp.exp2(lse - total)[:, half(hd)]
        return out.T.astype(BF16)

    for hd in range(2):
        for n, tile, lse in ((0, 2, theirs(0, 3)), (1, 5, theirs(1, 7))):
            cbuf[n, :, hd * HEAD:(hd + 1) * HEAD] = joined(tile, n, hd, side_total[n], lse)
            for e in (1, 2, 3, 0):
                send(("side", n, e, hd))
    for hd in range(2):
        for r, n, lse in ((1, 2, theirs(0, 6)), (0, 3, theirs(1, 1))):
            obuf[r, :, hd * HEAD:(hd + 1) * HEAD] = joined(4 * r, n, hd, own_total[r], lse)
            for e in range(4):
                if r or e:
                    send(("line", r, e, hd))

    cols = pl.ds(pl.multiple_of((2 * g + c) * 2 * HEAD, 2 * HEAD), 2 * HEAD)
    abuf[:, cols] = obuf[0, pl.ds(pl.multiple_of(g * 32, 32), 32), :]
    drain(recv_slot("lx"), 8)
    for hd in range(2):
        lse_ref[pl.ds(2 * other + hd, 1), :] = lxr[hd, 0:1, :]
    drain(recv_slot("line"), 224)
    drain(recv_slot("side"), 256)
    attn_ref[...] = (abuf[...].astype(F32) + abufc[...].astype(F32)).astype(BF16)
    for group, kib in enumerate((28 * 64, 16 * 64, 8 * 64 + 256, 256)):
        drain(send_sem.at[group], kib)


def settle(attn_in, lse_in, attn_out, lse_out, sem):
    copies = [
        pltpu.make_async_copy(attn_in, attn_out, sem.at[0]),
        pltpu.make_async_copy(lse_in, lse_out, sem.at[1]),
    ]
    for copy in copies:
        copy.start()
    for copy in copies:
        copy.wait()


def local(queries, keys, values, block_order):
    hbm = pl.BlockSpec(memory_space=pltpu.HBM)
    vmem = pl.BlockSpec(memory_space=pltpu.VMEM)
    results = pl.pallas_call(
        kernel,
        out_shape=(
            jax.ShapeDtypeStruct((32, 4096), BF16),
            jax.ShapeDtypeStruct((4, ROWS), F32),
        ),
        in_specs=[hbm, hbm, hbm, hbm],
        out_specs=(vmem, vmem),
        scratch_shapes=[
            pltpu.VMEM((8, 256, HEAD), BF16),
            pltpu.VMEM((8, 256, HEAD), BF16),
            pltpu.VMEM((8, HEAD, 256), BF16),
            pltpu.VMEM((ROWS, 2 * HEAD), BF16),
            pltpu.VMEM((HEAD, ROWS), BF16),
            pltpu.VMEM((8, 8, HEAD), jnp.int32),
            pltpu.VMEM((8, HEAD, 256), F32),
            pltpu.VMEM((8, 8, 256), F32),
            pltpu.VMEM((8, 8, 256), F32),
            pltpu.VMEM((8, HEAD, ROWS), BF16),
            pltpu.VMEM((8, HEAD), F32),
            pltpu.VMEM((8, HEAD, ROWS), BF16),
            pltpu.VMEM((3, 8, HEAD), F32),
            pltpu.VMEM((2, ROWS, 2 * HEAD), BF16),
            pltpu.VMEM((32, 4096), BF16),
            pltpu.VMEM((2, ROWS, 2 * HEAD), BF16),
            pltpu.VMEM((32, 4096), BF16),
            pltpu.VMEM((2, 8, ROWS), F32),
            pltpu.VMEM((2, 8, ROWS), F32),
            pltpu.VMEM((512, HEAD), F32),
            pltpu.VMEM((512, HEAD), F32),
            pltpu.VMEM((512, HEAD), BF16),
            pltpu.VMEM((512, HEAD), BF16),
            pltpu.VMEM((ROWS, HEAD), BF16),
            pltpu.VMEM((ROWS, 2 * HEAD), BF16),
            pltpu.VMEM((448, 8, ROWS), F32),
            pltpu.SMEM((128,), jnp.int32),
            pltpu.SemaphoreType.DMA((7,)),
            pltpu.SemaphoreType.DMA((4,)),
            pltpu.SemaphoreType.DMA((50,)),
        ],
        compiler_params=pltpu.CompilerParams(collective_id=0, has_side_effects=True, vmem_limit_bytes=24 * 1024 * 1024),
        name="attention",
    )(*[pltpu.with_memory_space_constraint(a, pltpu.HBM) for a in (queries, keys, values, block_order)])
    return pl.pallas_call(
        settle,
        out_shape=(
            jax.ShapeDtypeStruct((32, 4096), BF16),
            jax.ShapeDtypeStruct((4, ROWS), F32),
        ),
        in_specs=[vmem, vmem],
        out_specs=(hbm, hbm),
        scratch_shapes=[pltpu.SemaphoreType.DMA((2,))],
        compiler_params=pltpu.CompilerParams(vmem_limit_bytes=2 * 1024 * 1024),
        name="settle",
    )(*results)


def solution(mesh):
    in_specs = (P("seq", "head"), P("seq", "head"), P("seq", "head"), P())
    out_specs = (P(("seq", "head"), None), P("head", "seq"))
    return jax.shard_map(local, mesh=mesh, in_specs=in_specs, out_specs=out_specs, check_vma=False)
```

```python
import functools

import jax
import jax.numpy as jnp
from jax import lax
from jax.experimental import pallas as pl
from jax.experimental.pallas import tpu as pltpu
from jax.sharding import PartitionSpec as P

MESH = pl.DeviceIdType.MESH
HEAD = 256
ROWS = 128
BLK = 64
NZ, NY = 8, 4
NEG = -1e30
BIG = 1e30
SCALE = 1.4426950408889634 / 16.0
FLOOR = -1e6
LN2 = 0.6931471805599453
F32 = jnp.float32
BF16 = jnp.bfloat16

RIGHT_SLOTS = (0, 1, 2, 3, 7)
LEFT_SLOTS = (0, 4, 5, 6, 7)
SLOT_DZ = (0, -1, -2, -3, 1, 2, 3, 4)
QUERY_DY = (0, -1, 1, 2)


def log_total(rows):
    top = functools.reduce(jnp.maximum, rows)
    return top + jnp.log2(functools.reduce(jnp.add, [jnp.exp2(row - top) for row in rows]))


def kernel(q_ref, k_ref, v_ref, order_hbm, attn_ref, lse_ref,
           qbuf, kbuf, vbuf, vm, vsw, qpos, acc, mx, ls,
           osend, lstat, orecv, lgot, cbuf, abufc, obuf, abuf, lxs, lxr, sa, sb, pa, pb, km, qm, yard, order_ref,
           local_sem, send_sem, recv_sem):
    s = lax.axis_index("seq")
    g = lax.axis_index("head")
    z = s // (2 * NY)
    y = (s // 2) % NY
    c = s % 2

    def at(dz, dy):
        return (((z + dz + NZ) % NZ) * NY + (y + dy + NY) % NY) * 2 + c

    partner = (s + 1 - 2 * c, g)
    up, down = (at(1, 0), g), (at(-1, 0), g)
    fore, back = (at(0, 1), g), (at(0, -1), g)

    loads = [
        pltpu.make_async_copy(v_ref, vm, local_sem.at[0]),
        pltpu.make_async_copy(k_ref.at[:, pl.ds(pl.multiple_of(c * HEAD, HEAD), HEAD)], kbuf.at[0, pl.ds(0, ROWS), :], local_sem.at[1]),
    ]
    for hd in range(2):
        loads.append(pltpu.make_async_copy(
            q_ref.at[:, pl.ds(pl.multiple_of(c * 2 * HEAD + hd * HEAD, HEAD), HEAD)],
            qbuf.at[0, pl.ds(hd * ROWS, ROWS), :], local_sem.at[2 + hd]))
    loads += [
        pltpu.make_async_copy(k_ref.at[:, pl.ds(pl.multiple_of((1 - c) * HEAD, HEAD), HEAD)], km, local_sem.at[4]),
        pltpu.make_async_copy(q_ref.at[:, pl.ds(pl.multiple_of((1 - c) * 2 * HEAD, HEAD), 2 * HEAD)], qm, local_sem.at[5]),
    ]
    order_load = pltpu.make_async_copy(order_hbm, order_ref, local_sem.at[6])
    loads[1].start()

    def across(index):
        return index + 1 - 2 * c

    far = (at(0, 2), g)
    members = (g, g + 1 - 2 * (g % 2), (g + 2) % 4, 3 - g)
    peers = [up, down, fore, back]
    for e in range(4):
        peers.append((across(s), members[e]))
        if e:
            peers.append((s, members[e]))
    barrier = pltpu.get_barrier_semaphore()
    for peer in peers:
        pl.semaphore_signal(barrier, inc=1, device_id=peer, device_id_type=MESH)
    for n in (4, 2, 3, 0, 5):
        loads[n].start()
    order_load.start()

    table = {}
    recv_slots = {}

    def recv_slot(key):
        return recv_sem.at[recv_slots.setdefault(key, len(recv_slots))]

    def message(name, src, dst, device, group, key=None):
        table[name] = pltpu.make_async_remote_copy(
            src_ref=src, dst_ref=dst, send_sem=send_sem.at[group], recv_sem=recv_slot(name if key is None else key),
            device_id=device, device_id_type=MESH)

    def drain(sem, kib):
        ref = yard.at[pl.ds(0, kib // 4)]
        pltpu.make_async_copy(ref, ref, sem).wait()

    other = 1 - c
    for hd in range(2):
        message(("xq", hd), qm.at[:, pl.ds(hd * HEAD, HEAD)], qbuf.at[4, pl.ds(hd * ROWS, ROWS), :], partner, 1)
    message("xk", km, kbuf.at[0, pl.ds(ROWS, ROWS), :], partner, 1)
    message("xv", vsw, vbuf.at[0, :, pl.ds(ROWS, ROWS)], partner, 1)
    for h in range(2):
        for p in range(2):
            def kpart(slot):
                return kbuf.at[slot, pl.ds(h * ROWS + p * BLK, BLK), :]

            def vpart(slot):
                return vbuf.at[slot, pl.ds(p * ROWS, ROWS), pl.ds(h * ROWS, ROWS)]

            for t in range(1, 5):
                key = ("end", h) if t == 4 else None
                message(("rk", h, t, p), kpart(RIGHT_SLOTS[t - 1]), kpart(RIGHT_SLOTS[t]), up, 0, key)
                message(("lv", h, t, p), vpart(LEFT_SLOTS[t - 1]), vpart(LEFT_SLOTS[t]), down, 0, key)
                if t < 4:
                    key_k, key_v = (("third_k", h), ("third_v", h)) if t == 3 else (None, None)
                    message(("lk", h, t, p), kpart(LEFT_SLOTS[t - 1]), kpart(LEFT_SLOTS[t]), down, 0, key_k)
                    message(("rv", h, t, p), vpart(RIGHT_SLOTS[t - 1]), vpart(RIGHT_SLOTS[t]), up, 0, key_v)

        def qpart(slot, hd):
            return qbuf.at[h * 4 + slot, pl.ds(hd * ROWS, ROWS), :]

        message(("qr", h, 0), qpart(0, 0), qpart(1, 0), fore, 1)
        message(("ql", h, 1), qpart(0, 1), qpart(2, 1), back, 1)
        message(("qr", h, 1), qpart(0, 1), qpart(1, 1), fore, 1, ("near", h))
        message(("ql", h, 0), qpart(0, 0), qpart(2, 0), back, 1, ("near", h))
        message(("qrr", h), qpart(1, 0), qpart(3, 0), fore, 1, ("far", h))
        message(("qll", h), qpart(2, 1), qpart(3, 1), back, 1, ("far", h))
    for n in range(4):
        for hd in range(2):
            message(("o", n, hd), osend.at[2 * n + hd], orecv.at[2 * n + hd], fore if n % 2 == 0 else back, 2)
    for n, device in enumerate((fore, back, far)):
        message(("stat", n), lstat, lgot.at[n], device, 3, "stat")
    for hd in range(2):
        message(("lx", hd), lxs.at[hd], lxr.at[hd], partner, 3, "lx")
    for hd in range(2):
        cols = pl.ds(pl.multiple_of(((2 * g + c) * 2 + hd) * HEAD, HEAD), HEAD)
        half_cols = pl.ds(hd * HEAD, HEAD)
        for e in range(4):
            there = members[e]
            rows = pl.ds(pl.multiple_of(there * 32, 32), 32)
            for n, target in enumerate((at(0, 1), across(at(0, -1)))):
                message(("side", n, e, hd), cbuf.at[n, rows, half_cols], abufc.at[:, cols], (target, there), 2, "side")
            for r, target in enumerate((s, across(s))):
                if r or e:
                    message(("line", r, e, hd), obuf.at[r, rows, half_cols], abuf.at[:, cols], (target, there), 3, "line")

    def send(name):
        table[name].start()

    def arrive(name):
        table[name].wait_recv()

    def key_bases(slot):
        out = []
        for h in range(2):
            origin = (((z + SLOT_DZ[slot] + NZ) % NZ) * NY + y) * 2 + (c if h == 0 else other)
            out += [order_ref[2 * origin] * BLK, order_ref[2 * origin + 1] * BLK]
        return out

    iota = lax.broadcasted_iota(jnp.int32, (BLK, HEAD), 0)

    score_buffers, weight_buffers = (sa, sb), (pa, pb)
    bases_of = {}
    queue = []
    count = [0]

    def stage_scores(item):
        i, slots = item["tile"], item["slots"]
        into = score_buffers[item["turn"] % 2]
        q = qbuf[i]
        for n, slot in enumerate(slots):
            into[n * 256:(n + 1) * 256, :] = lax.dot_general(
                kbuf[slot], q, (((1,), (1,)), ((), ())), preferred_element_type=F32)

    def stage_weights(item):
        i, slots = item["tile"], item["slots"]
        source, into = score_buffers[item["turn"] % 2], weight_buffers[item["turn"] % 2]
        diagonal = slots == (0,) and i in (0, 4)
        first = slots == (0,)
        position = qpos[i, 0:1, :]
        for slot in slots:
            if slot not in bases_of:
                bases_of[slot] = key_bases(slot)
        bases = [base for slot in slots for base in bases_of[slot]]

        def raw(b):
            block = source[b * BLK:(b + 1) * BLK, :]
            return jnp.where(iota <= position - bases[b], block, NEG) if diagonal else block

        old = jnp.full((1, HEAD), FLOOR, F32) if first else mx[i, 0:1, :]
        allowed = [base <= position for base in bases]
        best = functools.reduce(jnp.maximum, [
            jnp.where(allowed[b], jnp.max(raw(b).reshape(8, 8, HEAD), axis=0), NEG) for b in range(len(bases))])
        best = jnp.max(best, axis=0, keepdims=True) * SCALE
        fresh = jnp.maximum(old, best)
        sums = None
        for b in range(len(bases)):
            weights = jnp.exp2(raw(b) * SCALE - jnp.where(allowed[b], fresh, BIG))
            part = jnp.sum(weights.reshape(8, 8, HEAD), axis=0)
            sums = part if sums is None else sums + part
            into[b * BLK:(b + 1) * BLK, :] = weights.astype(BF16)
        if first:
            item["factor"] = None
        else:
            item["factor"] = jnp.exp2(old - fresh)
            sums = ls[i] * item["factor"] + sums
        if item["last"]:
            item["top"], item["sums"] = fresh, sums
        else:
            mx[i] = jnp.broadcast_to(fresh, (8, HEAD))
            ls[i] = sums

    def stage_values(item):
        i, slots = item["tile"], item["slots"]
        source = weight_buffers[item["turn"] % 2]
        update = functools.reduce(jnp.add, [
            lax.dot_general(vbuf[slot], source[n * 256:(n + 1) * 256, :], (((1,), (0,)), ((), ())), preferred_element_type=F32)
            for n, slot in enumerate(slots)
        ])
        if item["factor"] is not None:
            update = acc[i] * item["factor"] + update
        if item["last"]:
            l = jnp.sum(item["sums"], axis=0, keepdims=True)
            some = l > 0.0
            inverse = jnp.where(some, 1.0 / jnp.where(some, l, 1.0), 0.0)
            item["done"](update * inverse, jnp.where(some, item["top"] + jnp.log2(jnp.where(some, l, 1.0)), NEG))
        else:
            acc[i] = update

    def advance():
        if queue and queue[-1]["stage"] == 0:
            stage_scores(queue[-1])
        for item in queue[::-1]:
            if item["stage"] == 1:
                stage_weights(item)
            elif item["stage"] == 2:
                stage_values(item)
        for item in queue:
            item["stage"] += 1
        queue[:] = [item for item in queue if item["stage"] < 3]

    def push(tiles, slots, done=None):
        for i in tiles:
            queue.append({"tile": i, "slots": slots, "turn": count[0], "stage": 0, "last": done is not None, "done": done})
            count[0] += 1
            advance()

    def flush():
        while queue:
            advance()

    def first_hop(kind, h):
        for p in range(2):
            send(("r" + kind, h, 1, p))
            send(("l" + kind, h, 1, p))

    def last_hop(h, p):
        send(("rk", h, 4, p))
        send(("lv", h, 4, p))

    def ring_keys(h, t):
        for p in range(2):
            arrive(("rk", h, t, p))
            if (h, t) != (0, 3):
                send(("rk", h, t + 1, p))
            if t < 3:
                arrive(("lk", h, t, p))
                send(("lk", h, t + 1, p))
        if t == 3:
            drain(recv_slot(("third_k", h)), 64)

    def ring_values(h, t):
        for p in range(2):
            arrive(("lv", h, t, p))
            if (h, t) != (0, 3):
                send(("lv", h, t + 1, p))
            if t < 3:
                arrive(("rv", h, t, p))
                send(("rv", h, t + 1, p))
        if t == 3:
            drain(recv_slot(("third_v", h)), 64)

    def ring_end(h):
        drain(recv_slot(("end", h)), 128)

    def spread(hd):
        arrive(("xq", hd))
        send(("qr", 1, hd))
        send(("ql", 1, hd))

    def relay(h):
        arrive(("qr", h, 0))
        send(("qrr", h))
        arrive(("ql", h, 1))
        send(("qll", h))
        drain(recv_slot(("near", h)), 128)

    def relayed(h):
        drain(recv_slot(("far", h)), 128)

    def cross_values():
        arrive("xv")
        first_hop("v", 1)

    def cross_keys():
        arrive("xk")
        first_hop("k", 1)

    assert len(recv_slots) == 70, len(recv_slots)
    loads[1].wait()
    loads[4].wait()
    pl.semaphore_wait(barrier, len(peers))
    first_hop("k", 0)
    send("xk")
    for hd in range(2):
        loads[2 + hd].wait()
        send(("qr", 0, hd))
        send(("ql", 0, hd))

    def flipped(column):
        v = vm[:, pl.ds(pl.multiple_of(column * HEAD, HEAD), HEAD)]
        return v.astype(F32).T.astype(BF16)

    loads[0].wait()
    vbuf[0, :, 0:ROWS] = flipped(c)
    vsw[...] = flipped(other)
    order_load.wait()
    lane = lax.broadcasted_iota(jnp.int32, (8, HEAD), 1)
    for slot in range(4):
        for h in range(2):
            origin = (z * NY + (y + QUERY_DY[slot] + NY) % NY) * 2 + (c if h == 0 else other)
            first, second = order_ref[2 * origin] * BLK, order_ref[2 * origin + 1] * BLK
            inside = lane % ROWS
            qpos[h * 4 + slot] = jnp.where(inside < BLK, first + inside, second + inside - BLK)
    send("xv")
    first_hop("v", 0)
    loads[5].wait()
    send(("xq", 0))
    send(("xq", 1))

    ring_keys(0, 1)
    cross_keys()
    relay(0)
    ring_values(0, 1)
    cross_values()
    push((0, 1, 2), (0,))
    spread(0)
    spread(1)
    ring_keys(0, 2)
    relayed(0)
    push((3,), (0,))
    ring_keys(1, 1)
    push((4,), (0,))
    ring_values(0, 2)
    ring_values(1, 1)
    push((0, 1), (1, 4))
    relay(1)
    push((2, 3), (1, 4))
    ring_keys(0, 3)
    push((5, 6), (0,))
    push((4, 5), (1, 4))
    ring_keys(1, 2)
    ring_values(0, 3)
    push((6,), (1, 4))
    ring_values(1, 2)
    for p in range(2):
        last_hop(0, p)
    relayed(1)
    push((7,), (0,))
    push((7,), (1, 4))
    push((0, 1), (2, 5))
    ring_keys(1, 3)
    push((2, 3, 4), (2, 5))
    ring_values(1, 3)
    push((5, 6, 7), (2, 5))
    push((0, 1, 2, 3, 4, 5, 6, 7), (3, 6))
    ring_end(0)
    ring_end(1)

    def half(hd):
        return slice(hd * ROWS, (hd + 1) * ROWS)

    direct = {3: 0, 7: 1, 6: 2, 1: 3}

    def done_with(tile):
        def done(o, lse):
            lstat[tile:tile + 1, :] = lse
            if tile in direct:
                n = direct[tile]
                for hd in range(2):
                    osend[2 * n + hd] = o[:, half(hd)].astype(BF16)
                    if n < 2 and hd == 0:
                        send(("o", n, hd))
            else:
                acc[tile] = o
        return done

    for tile in (3, 7, 6, 1, 2, 5, 0, 4):
        push((tile,), (7,), done_with(tile))
    flush()
    for n in range(3):
        send(("stat", n))
    for n, hd in ((0, 1), (1, 1), (2, 0), (3, 0), (2, 1), (3, 1)):
        send(("o", n, hd))
    drain(recv_slot("stat"), 24)

    def mine(i):
        return lstat[i:i + 1, :]

    def theirs(n, i):
        return lgot[n, i:i + 1, :]

    side_total = [
        log_total([mine(2), theirs(0, 3), theirs(1, 0), theirs(2, 1)]),
        log_total([mine(5), theirs(1, 7), theirs(0, 4), theirs(2, 6)]),
    ]
    own_total = [log_total([mine(4 * h), theirs(0, 4 * h + 2), theirs(1, 4 * h + 1), theirs(2, 4 * h + 3)]) for h in range(2)]
    for hd in range(2):
        lxs[hd] = jnp.broadcast_to(own_total[1][:, half(hd)] * LN2, (8, ROWS))
        send(("lx", hd))
        lse_ref[pl.ds(2 * c + hd, 1), :] = own_total[0][:, half(hd)] * LN2

    def joined(tile, n, hd, total, lse):
        arrive(("o", n, hd))
        out = acc[tile, :, half(hd)] * jnp.exp2(mine(tile) - total)[:, half(hd)]
        out = out + orecv[2 * n + hd].astype(F32) * jnp.exp2(lse - total)[:, half(hd)]
        return out.T.astype(BF16)

    for hd in range(2):
        for n, tile, lse in ((0, 2, theirs(0, 3)), (1, 5, theirs(1, 7))):
            cbuf[n, :, hd * HEAD:(hd + 1) * HEAD] = joined(tile, n, hd, side_total[n], lse)
            for e in (2, 3, 1, 0) if n == 0 else (0, 1, 2, 3):
                send(("side", n, e, hd))
    for hd in range(2):
        for r, n, lse in ((1, 2, theirs(0, 6)), (0, 3, theirs(1, 1))):
            obuf[r, :, hd * HEAD:(hd + 1) * HEAD] = joined(4 * r, n, hd, own_total[r], lse)
            for e in (0, 1, 2, 3) if r else (2, 3, 1):
                send(("line", r, e, hd))

    cols = pl.ds(pl.multiple_of((2 * g + c) * 2 * HEAD, 2 * HEAD), 2 * HEAD)
    abuf[:, cols] = obuf[0, pl.ds(pl.multiple_of(g * 32, 32), 32), :]
    drain(recv_slot("lx"), 8)
    for hd in range(2):
        lse_ref[pl.ds(2 * other + hd, 1), :] = lxr[hd, 0:1, :]
    drain(recv_slot("line"), 224)
    drain(recv_slot("side"), 256)
    attn_ref[...] = (abuf[...].astype(F32) + abufc[...].astype(F32)).astype(BF16)
    for group, kib in enumerate((28 * 64, 16 * 64, 8 * 64 + 256, 256)):
        drain(send_sem.at[group], kib)


def settle(attn_in, lse_in, attn_out, lse_out, sem):
    copies = [
        pltpu.make_async_copy(attn_in, attn_out, sem.at[0]),
        pltpu.make_async_copy(lse_in, lse_out, sem.at[1]),
    ]
    for copy in copies:
        copy.start()
    for copy in copies:
        copy.wait()


def local(queries, keys, values, block_order):
    hbm = pl.BlockSpec(memory_space=pltpu.HBM)
    vmem = pl.BlockSpec(memory_space=pltpu.VMEM)
    results = pl.pallas_call(
        kernel,
        out_shape=(
            jax.ShapeDtypeStruct((32, 4096), BF16),
            jax.ShapeDtypeStruct((4, ROWS), F32),
        ),
        in_specs=[hbm, hbm, hbm, hbm],
        out_specs=(vmem, vmem),
        scratch_shapes=[
            pltpu.VMEM((8, 256, HEAD), BF16),
            pltpu.VMEM((8, 256, HEAD), BF16),
            pltpu.VMEM((8, HEAD, 256), BF16),
            pltpu.VMEM((ROWS, 2 * HEAD), BF16),
            pltpu.VMEM((HEAD, ROWS), BF16),
            pltpu.VMEM((8, 8, HEAD), jnp.int32),
            pltpu.VMEM((8, HEAD, 256), F32),
            pltpu.VMEM((8, 8, 256), F32),
            pltpu.VMEM((8, 8, 256), F32),
            pltpu.VMEM((8, HEAD, ROWS), BF16),
            pltpu.VMEM((8, HEAD), F32),
            pltpu.VMEM((8, HEAD, ROWS), BF16),
            pltpu.VMEM((3, 8, HEAD), F32),
            pltpu.VMEM((2, ROWS, 2 * HEAD), BF16),
            pltpu.VMEM((32, 4096), BF16),
            pltpu.VMEM((2, ROWS, 2 * HEAD), BF16),
            pltpu.VMEM((32, 4096), BF16),
            pltpu.VMEM((2, 8, ROWS), F32),
            pltpu.VMEM((2, 8, ROWS), F32),
            pltpu.VMEM((512, HEAD), F32),
            pltpu.VMEM((512, HEAD), F32),
            pltpu.VMEM((512, HEAD), BF16),
            pltpu.VMEM((512, HEAD), BF16),
            pltpu.VMEM((ROWS, HEAD), BF16),
            pltpu.VMEM((ROWS, 2 * HEAD), BF16),
            pltpu.VMEM((448, 8, ROWS), F32),
            pltpu.SMEM((128,), jnp.int32),
            pltpu.SemaphoreType.DMA((7,)),
            pltpu.SemaphoreType.DMA((4,)),
            pltpu.SemaphoreType.DMA((70,)),
        ],
        compiler_params=pltpu.CompilerParams(collective_id=0, has_side_effects=True, vmem_limit_bytes=24 * 1024 * 1024),
        name="attention",
    )(*[pltpu.with_memory_space_constraint(a, pltpu.HBM) for a in (queries, keys, values, block_order)])
    return pl.pallas_call(
        settle,
        out_shape=(
            jax.ShapeDtypeStruct((32, 4096), BF16),
            jax.ShapeDtypeStruct((4, ROWS), F32),
        ),
        in_specs=[vmem, vmem],
        out_specs=(hbm, hbm),
        scratch_shapes=[pltpu.SemaphoreType.DMA((2,))],
        compiler_params=pltpu.CompilerParams(vmem_limit_bytes=2 * 1024 * 1024),
        name="settle",
    )(*results)


def solution(mesh):
    in_specs = (P("seq", "head"), P("seq", "head"), P("seq", "head"), P())
    out_specs = (P(("seq", "head"), None), P("head", "seq"))
    return jax.shard_map(local, mesh=mesh, in_specs=in_specs, out_specs=out_specs, check_vma=False)
```

```python
import functools

import jax
import jax.numpy as jnp
from jax import lax
from jax.experimental import pallas as pl
from jax.experimental.pallas import tpu as pltpu
from jax.sharding import PartitionSpec as P

MESH = pl.DeviceIdType.MESH
HEAD = 256
ROWS = 128
BLK = 64
NZ, NY = 8, 4
NEG = -1e30
BIG = 1e30
SCALE = 1.4426950408889634 / 16.0
FLOOR = -1e6
LN2 = 0.6931471805599453
F32 = jnp.float32
BF16 = jnp.bfloat16

RIGHT_SLOTS = (0, 1, 2, 3, 7)
LEFT_SLOTS = (0, 4, 5, 6, 7)
SLOT_DZ = (0, -1, -2, -3, 1, 2, 3, 4)
QUERY_DY = (0, -1, 1, 2)


def log_total(rows):
    top = functools.reduce(jnp.maximum, rows)
    return top + jnp.log2(functools.reduce(jnp.add, [jnp.exp2(row - top) for row in rows]))


def kernel(q_ref, k_ref, v_ref, order_hbm, attn_ref, lse_ref,
           qbuf, kbuf, vbuf, vm, vsw, qpos, acc, mx, ls,
           osend, lstat, orecv, lgot, cbuf, abufc, obuf, abuf, lxs, lxr, sa, sb, pa, pb, km, qm, yard, order_ref,
           local_sem, send_sem, recv_sem):
    s = lax.axis_index("seq")
    g = lax.axis_index("head")
    z = s // (2 * NY)
    y = (s // 2) % NY
    c = s % 2

    def at(dz, dy):
        return (((z + dz + NZ) % NZ) * NY + (y + dy + NY) % NY) * 2 + c

    partner = (s + 1 - 2 * c, g)
    up, down = (at(1, 0), g), (at(-1, 0), g)
    fore, back = (at(0, 1), g), (at(0, -1), g)

    loads = [
        pltpu.make_async_copy(v_ref, vm, local_sem.at[0]),
        pltpu.make_async_copy(k_ref.at[:, pl.ds(pl.multiple_of(c * HEAD, HEAD), HEAD)], kbuf.at[0, pl.ds(0, ROWS), :], local_sem.at[1]),
    ]
    for hd in range(2):
        loads.append(pltpu.make_async_copy(
            q_ref.at[:, pl.ds(pl.multiple_of(c * 2 * HEAD + hd * HEAD, HEAD), HEAD)],
            qbuf.at[0, pl.ds(hd * ROWS, ROWS), :], local_sem.at[2 + hd]))
    loads += [
        pltpu.make_async_copy(k_ref.at[:, pl.ds(pl.multiple_of((1 - c) * HEAD, HEAD), HEAD)], km, local_sem.at[4]),
        pltpu.make_async_copy(q_ref.at[:, pl.ds(pl.multiple_of((1 - c) * 2 * HEAD, HEAD), 2 * HEAD)], qm, local_sem.at[5]),
    ]
    order_load = pltpu.make_async_copy(order_hbm, order_ref, local_sem.at[6])
    loads[1].start()

    def across(index):
        return index + 1 - 2 * c

    far = (at(0, 2), g)
    members = (g, g + 1 - 2 * (g % 2), (g + 2) % 4, 3 - g)
    peers = [up, down, fore, back]
    for e in range(4):
        peers.append((across(s), members[e]))
        if e:
            peers.append((s, members[e]))
    barrier = pltpu.get_barrier_semaphore()
    for peer in peers:
        pl.semaphore_signal(barrier, inc=1, device_id=peer, device_id_type=MESH)
    for n in (4, 2, 3, 0, 5):
        loads[n].start()
    order_load.start()

    table = {}
    recv_slots = {}

    def recv_slot(key):
        return recv_sem.at[recv_slots.setdefault(key, len(recv_slots))]

    def message(name, src, dst, device, group, key=None):
        table[name] = pltpu.make_async_remote_copy(
            src_ref=src, dst_ref=dst, send_sem=send_sem.at[group], recv_sem=recv_slot(name if key is None else key),
            device_id=device, device_id_type=MESH)

    def drain(sem, kib):
        ref = yard.at[pl.ds(0, kib // 4)]
        pltpu.make_async_copy(ref, ref, sem).wait()

    other = 1 - c
    for hd in range(2):
        message(("xq", hd), qm.at[:, pl.ds(hd * HEAD, HEAD)], qbuf.at[4, pl.ds(hd * ROWS, ROWS), :], partner, 1)
    message("xk", km, kbuf.at[0, pl.ds(ROWS, ROWS), :], partner, 1)
    message("xv", vsw, vbuf.at[0, :, pl.ds(ROWS, ROWS)], partner, 1)
    for h in range(2):
        for p in range(2):
            def kpart(slot):
                return kbuf.at[slot, pl.ds(h * ROWS + p * BLK, BLK), :]

            def vpart(slot):
                return vbuf.at[slot, pl.ds(p * ROWS, ROWS), pl.ds(h * ROWS, ROWS)]

            for t in range(1, 5):
                key_k, key_v = (("end", h), ("end", h)) if t == 4 else (("k", h, t, p), ("v", h, t, p))
                message(("rk", h, t, p), kpart(RIGHT_SLOTS[t - 1]), kpart(RIGHT_SLOTS[t]), up, 0, key_k)
                message(("lv", h, t, p), vpart(LEFT_SLOTS[t - 1]), vpart(LEFT_SLOTS[t]), down, 0, key_v)
                if t < 4:
                    message(("lk", h, t, p), kpart(LEFT_SLOTS[t - 1]), kpart(LEFT_SLOTS[t]), down, 0, key_k)
                    message(("rv", h, t, p), vpart(RIGHT_SLOTS[t - 1]), vpart(RIGHT_SLOTS[t]), up, 0, key_v)

        def qpart(slot, hd):
            return qbuf.at[h * 4 + slot, pl.ds(hd * ROWS, ROWS), :]

        message(("qr", h, 0), qpart(0, 0), qpart(1, 0), fore, 1, ("pass", h))
        message(("ql", h, 1), qpart(0, 1), qpart(2, 1), back, 1, ("pass", h))
        message(("qr", h, 1), qpart(0, 1), qpart(1, 1), fore, 1, ("near", h))
        message(("ql", h, 0), qpart(0, 0), qpart(2, 0), back, 1, ("near", h))
        message(("qrr", h), qpart(1, 0), qpart(3, 0), fore, 1, ("far", h))
        message(("qll", h), qpart(2, 1), qpart(3, 1), back, 1, ("far", h))
    for n in range(4):
        for hd in range(2):
            message(("o", n, hd), osend.at[2 * n + hd], orecv.at[2 * n + hd], fore if n % 2 == 0 else back, 2, ("o", n // 2, hd))
    for n, device in enumerate((fore, back, far)):
        message(("stat", n), lstat, lgot.at[n], device, 3, "stat")
    for hd in range(2):
        message(("lx", hd), lxs.at[hd], lxr.at[hd], partner, 3, "lx")
    for hd in range(2):
        cols = pl.ds(pl.multiple_of(((2 * g + c) * 2 + hd) * HEAD, HEAD), HEAD)
        half_cols = pl.ds(hd * HEAD, HEAD)
        for e in range(4):
            there = members[e]
            rows = pl.ds(pl.multiple_of(there * 32, 32), 32)
            for n, target in enumerate((at(0, 1), across(at(0, -1)))):
                message(("side", n, e, hd), cbuf.at[n, rows, half_cols], abufc.at[:, cols], (target, there), 2, "side")
            for r, target in enumerate((s, across(s))):
                if r or e:
                    message(("line", r, e, hd), obuf.at[r, rows, half_cols], abuf.at[:, cols], (target, there), 3, "line")

    def send(name):
        table[name].start()

    def arrive(name):
        table[name].wait_recv()

    def key_bases(slot):
        out = []
        for h in range(2):
            origin = (((z + SLOT_DZ[slot] + NZ) % NZ) * NY + y) * 2 + (c if h == 0 else other)
            out += [order_ref[2 * origin] * BLK, order_ref[2 * origin + 1] * BLK]
        return out

    iota = lax.broadcasted_iota(jnp.int32, (BLK, HEAD), 0)

    score_buffers, weight_buffers = (sa, sb), (pa, pb)
    bases_of = {}
    queue = []
    count = [0]

    def stage_scores(item):
        i, slots = item["tile"], item["slots"]
        into = score_buffers[item["turn"] % 2]
        q = qbuf[i]
        for n, slot in enumerate(slots):
            into[n * 256:(n + 1) * 256, :] = lax.dot_general(
                kbuf[slot], q, (((1,), (1,)), ((), ())), preferred_element_type=F32)

    def stage_weights(item):
        i, slots = item["tile"], item["slots"]
        source, into = score_buffers[item["turn"] % 2], weight_buffers[item["turn"] % 2]
        diagonal = slots == (0,) and i in (0, 4)
        first = slots == (0,)
        position = qpos[i, 0:1, :]
        for slot in slots:
            if slot not in bases_of:
                bases_of[slot] = key_bases(slot)
        bases = [base for slot in slots for base in bases_of[slot]]

        def raw(b):
            block = source[b * BLK:(b + 1) * BLK, :]
            return jnp.where(iota <= position - bases[b], block, NEG) if diagonal else block

        old = jnp.full((1, HEAD), FLOOR, F32) if first else mx[i, 0:1, :]
        allowed = [base <= position for base in bases]
        best = functools.reduce(jnp.maximum, [
            jnp.where(allowed[b], jnp.max(raw(b).reshape(8, 8, HEAD), axis=0), NEG) for b in range(len(bases))])
        best = jnp.max(best, axis=0, keepdims=True) * SCALE
        fresh = jnp.maximum(old, best)
        sums = None
        for b in range(len(bases)):
            weights = jnp.exp2(raw(b) * SCALE - jnp.where(allowed[b], fresh, BIG))
            part = jnp.sum(weights.reshape(8, 8, HEAD), axis=0)
            sums = part if sums is None else sums + part
            into[b * BLK:(b + 1) * BLK, :] = weights.astype(BF16)
        if first:
            item["factor"] = None
        else:
            item["factor"] = jnp.exp2(old - fresh)
            sums = ls[i] * item["factor"] + sums
        if item["last"]:
            item["top"], item["sums"] = fresh, sums
        else:
            mx[i] = jnp.broadcast_to(fresh, (8, HEAD))
            ls[i] = sums

    def stage_values(item):
        i, slots = item["tile"], item["slots"]
        source = weight_buffers[item["turn"] % 2]
        update = functools.reduce(jnp.add, [
            lax.dot_general(vbuf[slot], source[n * 256:(n + 1) * 256, :], (((1,), (0,)), ((), ())), preferred_element_type=F32)
            for n, slot in enumerate(slots)
        ])
        if item["factor"] is not None:
            update = acc[i] * item["factor"] + update
        if item["last"]:
            l = jnp.sum(item["sums"], axis=0, keepdims=True)
            some = l > 0.0
            inverse = jnp.where(some, 1.0 / jnp.where(some, l, 1.0), 0.0)
            item["done"](update * inverse, jnp.where(some, item["top"] + jnp.log2(jnp.where(some, l, 1.0)), NEG))
        else:
            acc[i] = update

    def advance():
        if queue and queue[-1]["stage"] == 0:
            stage_scores(queue[-1])
        for item in queue[::-1]:
            if item["stage"] == 1:
                stage_weights(item)
            elif item["stage"] == 2:
                stage_values(item)
        for item in queue:
            item["stage"] += 1
        queue[:] = [item for item in queue if item["stage"] < 3]

    def push(tiles, slots, done=None):
        for i in tiles:
            queue.append({"tile": i, "slots": slots, "turn": count[0], "stage": 0, "last": done is not None, "done": done})
            count[0] += 1
            advance()

    def flush():
        while queue:
            advance()

    def first_hop(kind, h):
        for p in range(2):
            send(("r" + kind, h, 1, p))
            send(("l" + kind, h, 1, p))

    def last_hop(h, p):
        send(("rk", h, 4, p))
        send(("lv", h, 4, p))

    def ring_keys(h, t):
        for p in range(2):
            drain(recv_slot(("k", h, t, p)), 64)
            if (h, t) != (0, 3):
                send(("rk", h, t + 1, p))
            if t < 3:
                send(("lk", h, t + 1, p))

    def ring_values(h, t):
        for p in range(2):
            drain(recv_slot(("v", h, t, p)), 64)
            if (h, t) != (0, 3):
                send(("lv", h, t + 1, p))
            if t < 3:
                send(("rv", h, t + 1, p))

    def ring_end(h):
        drain(recv_slot(("end", h)), 128)

    def spread(hd):
        arrive(("xq", hd))
        send(("qr", 1, hd))
        send(("ql", 1, hd))

    def relay(h):
        drain(recv_slot(("pass", h)), 128)
        send(("qrr", h))
        send(("qll", h))
        drain(recv_slot(("near", h)), 128)

    def relayed(h):
        drain(recv_slot(("far", h)), 128)

    def cross_values():
        arrive("xv")
        first_hop("v", 1)

    def cross_keys():
        arrive("xk")
        first_hop("k", 1)

    assert len(recv_slots) == 44, len(recv_slots)
    loads[1].wait()
    loads[4].wait()
    pl.semaphore_wait(barrier, len(peers))
    first_hop("k", 0)
    send("xk")
    for hd in range(2):
        loads[2 + hd].wait()
        send(("qr", 0, hd))
        send(("ql", 0, hd))

    def flipped(column):
        v = vm[:, pl.ds(pl.multiple_of(column * HEAD, HEAD), HEAD)]
        return v.astype(F32).T.astype(BF16)

    loads[0].wait()
    vbuf[0, :, 0:ROWS] = flipped(c)
    vsw[...] = flipped(other)
    order_load.wait()
    lane = lax.broadcasted_iota(jnp.int32, (8, HEAD), 1)
    for slot in range(4):
        for h in range(2):
            origin = (z * NY + (y + QUERY_DY[slot] + NY) % NY) * 2 + (c if h == 0 else other)
            first, second = order_ref[2 * origin] * BLK, order_ref[2 * origin + 1] * BLK
            inside = lane % ROWS
            qpos[h * 4 + slot] = jnp.where(inside < BLK, first + inside, second + inside - BLK)
    send("xv")
    first_hop("v", 0)
    loads[5].wait()
    send(("xq", 0))
    send(("xq", 1))

    ring_keys(0, 1)
    cross_keys()
    relay(0)
    ring_values(0, 1)
    cross_values()
    push((0, 1, 2), (0,))
    spread(0)
    spread(1)
    ring_keys(1, 1)
    ring_keys(0, 2)
    relayed(0)
    push((3,), (0,))
    push((4,), (0,))
    ring_values(0, 2)
    ring_values(1, 1)
    push((0, 1), (1, 4))
    relay(1)
    push((2, 3), (1, 4))
    ring_keys(0, 3)
    push((5, 6), (0,))
    push((4, 5), (1, 4))
    ring_keys(1, 2)
    ring_values(0, 3)
    push((6,), (1, 4))
    ring_values(1, 2)
    for p in range(2):
        last_hop(0, p)
    relayed(1)
    push((7,), (0,))
    push((7,), (1, 4))
    push((0, 1), (2, 5))
    ring_keys(1, 3)
    push((2, 3, 4), (2, 5))
    ring_values(1, 3)
    push((5, 6, 7), (2, 5))
    push((0, 1, 2, 3, 4, 5, 6, 7), (3, 6))
    ring_end(0)
    ring_end(1)

    def half(hd):
        return slice(hd * ROWS, (hd + 1) * ROWS)

    direct = {3: 0, 7: 1, 6: 2, 1: 3}

    def done_with(tile):
        def done(o, lse):
            lstat[tile:tile + 1, :] = lse
            if tile in direct:
                n = direct[tile]
                for hd in range(2):
                    osend[2 * n + hd] = o[:, half(hd)].astype(BF16)
                    if n < 2 and hd == 0:
                        send(("o", n, hd))
            else:
                acc[tile] = o
        return done

    for tile in (3, 7, 6, 1, 2, 5, 0, 4):
        push((tile,), (7,), done_with(tile))
    flush()
    for n in range(3):
        send(("stat", n))
    for n, hd in ((0, 1), (1, 1), (2, 0), (3, 0), (2, 1), (3, 1)):
        send(("o", n, hd))
    drain(recv_slot("stat"), 24)

    def mine(i):
        return lstat[i:i + 1, :]

    def theirs(n, i):
        return lgot[n, i:i + 1, :]

    side_total = [
        log_total([mine(2), theirs(0, 3), theirs(1, 0), theirs(2, 1)]),
        log_total([mine(5), theirs(1, 7), theirs(0, 4), theirs(2, 6)]),
    ]
    own_total = [log_total([mine(4 * h), theirs(0, 4 * h + 2), theirs(1, 4 * h + 1), theirs(2, 4 * h + 3)]) for h in range(2)]
    for hd in range(2):
        lxs[hd] = jnp.broadcast_to(own_total[1][:, half(hd)] * LN2, (8, ROWS))
        send(("lx", hd))
        lse_ref[pl.ds(2 * c + hd, 1), :] = own_total[0][:, half(hd)] * LN2

    def joined(tile, n, hd, total, lse):
        out = acc[tile, :, half(hd)] * jnp.exp2(mine(tile) - total)[:, half(hd)]
        out = out + orecv[2 * n + hd].astype(F32) * jnp.exp2(lse - total)[:, half(hd)]
        return out.T.astype(BF16)

    for hd in range(2):
        drain(recv_slot(("o", 0, hd)), 128)
        for n, tile, lse in ((0, 2, theirs(0, 3)), (1, 5, theirs(1, 7))):
            cbuf[n, :, hd * HEAD:(hd + 1) * HEAD] = joined(tile, n, hd, side_total[n], lse)
            for e in (2, 3, 1, 0) if n == 0 else (0, 1, 2, 3):
                send(("side", n, e, hd))
    for hd in range(2):
        drain(recv_slot(("o", 1, hd)), 128)
        for r, n, lse in ((1, 2, theirs(0, 6)), (0, 3, theirs(1, 1))):
            obuf[r, :, hd * HEAD:(hd + 1) * HEAD] = joined(4 * r, n, hd, own_total[r], lse)
            for e in (0, 1, 2, 3) if r else (2, 3, 1):
                send(("line", r, e, hd))

    cols = pl.ds(pl.multiple_of((2 * g + c) * 2 * HEAD, 2 * HEAD), 2 * HEAD)
    abuf[:, cols] = obuf[0, pl.ds(pl.multiple_of(g * 32, 32), 32), :]
    drain(recv_slot("lx"), 8)
    for hd in range(2):
        lse_ref[pl.ds(2 * other + hd, 1), :] = lxr[hd, 0:1, :]
    drain(recv_slot("line"), 224)
    drain(recv_slot("side"), 256)
    attn_ref[...] = (abuf[...].astype(F32) + abufc[...].astype(F32)).astype(BF16)
    for group, kib in enumerate((28 * 64, 16 * 64, 8 * 64 + 256, 256)):
        drain(send_sem.at[group], kib)


def settle(attn_in, lse_in, attn_out, lse_out, sem):
    copies = [
        pltpu.make_async_copy(attn_in, attn_out, sem.at[0]),
        pltpu.make_async_copy(lse_in, lse_out, sem.at[1]),
    ]
    for copy in copies:
        copy.start()
    for copy in copies:
        copy.wait()


def local(queries, keys, values, block_order):
    hbm = pl.BlockSpec(memory_space=pltpu.HBM)
    vmem = pl.BlockSpec(memory_space=pltpu.VMEM)
    results = pl.pallas_call(
        kernel,
        out_shape=(
            jax.ShapeDtypeStruct((32, 4096), BF16),
            jax.ShapeDtypeStruct((4, ROWS), F32),
        ),
        in_specs=[hbm, hbm, hbm, hbm],
        out_specs=(vmem, vmem),
        scratch_shapes=[
            pltpu.VMEM((8, 256, HEAD), BF16),
            pltpu.VMEM((8, 256, HEAD), BF16),
            pltpu.VMEM((8, HEAD, 256), BF16),
            pltpu.VMEM((ROWS, 2 * HEAD), BF16),
            pltpu.VMEM((HEAD, ROWS), BF16),
            pltpu.VMEM((8, 8, HEAD), jnp.int32),
            pltpu.VMEM((8, HEAD, 256), F32),
            pltpu.VMEM((8, 8, 256), F32),
            pltpu.VMEM((8, 8, 256), F32),
            pltpu.VMEM((8, HEAD, ROWS), BF16),
            pltpu.VMEM((8, HEAD), F32),
            pltpu.VMEM((8, HEAD, ROWS), BF16),
            pltpu.VMEM((3, 8, HEAD), F32),
            pltpu.VMEM((2, ROWS, 2 * HEAD), BF16),
            pltpu.VMEM((32, 4096), BF16),
            pltpu.VMEM((2, ROWS, 2 * HEAD), BF16),
            pltpu.VMEM((32, 4096), BF16),
            pltpu.VMEM((2, 8, ROWS), F32),
            pltpu.VMEM((2, 8, ROWS), F32),
            pltpu.VMEM((512, HEAD), F32),
            pltpu.VMEM((512, HEAD), F32),
            pltpu.VMEM((512, HEAD), BF16),
            pltpu.VMEM((512, HEAD), BF16),
            pltpu.VMEM((ROWS, HEAD), BF16),
            pltpu.VMEM((ROWS, 2 * HEAD), BF16),
            pltpu.VMEM((448, 8, ROWS), F32),
            pltpu.SMEM((128,), jnp.int32),
            pltpu.SemaphoreType.DMA((7,)),
            pltpu.SemaphoreType.DMA((4,)),
            pltpu.SemaphoreType.DMA((44,)),
        ],
        compiler_params=pltpu.CompilerParams(collective_id=0, has_side_effects=True, vmem_limit_bytes=24 * 1024 * 1024),
        name="attention",
    )(*[pltpu.with_memory_space_constraint(a, pltpu.HBM) for a in (queries, keys, values, block_order)])
    return pl.pallas_call(
        settle,
        out_shape=(
            jax.ShapeDtypeStruct((32, 4096), BF16),
            jax.ShapeDtypeStruct((4, ROWS), F32),
        ),
        in_specs=[vmem, vmem],
        out_specs=(hbm, hbm),
        scratch_shapes=[pltpu.SemaphoreType.DMA((2,))],
        compiler_params=pltpu.CompilerParams(vmem_limit_bytes=2 * 1024 * 1024),
        name="settle",
    )(*results)


def solution(mesh):
    in_specs = (P("seq", "head"), P("seq", "head"), P("seq", "head"), P())
    out_specs = (P(("seq", "head"), None), P("head", "seq"))
    return jax.shard_map(local, mesh=mesh, in_specs=in_specs, out_specs=out_specs, check_vma=False)
```
